32 devices in a mesh: ens: 2 (over x), col: 4 (over z), row: 4 (over y, core).
Axes of the slice: x: 2, y: 2, z: 4, core: 2. Of those that a mesh axis runs over, the one named last changes fastest.
Arguments:
- u_init: float32 [8192, 4096], P(('ens', 'row'), 'col'), parts along dimension 0
- v_init: float32 [8192, 4096], P(('ens', 'row'), 'col'), parts along dimension 0
- stencil_w: float32 [48, 3, 3], replicated
Outputs:
- output 1: float32 [8192, 4096], P(('ens', 'row'), 'col'), parts along dimension 0
- output 2: float32 [8192, 4096], P(('ens', 'row'), 'col'), parts along dimension 0
There are 2 independent parts. The reference program is written for one: setup_inputs(seed, part) draws one part's arguments, and reference() takes and returns one part's arrays. A program takes and returns all parts, laid end to end along the dimension named above; an argument that names none is the same for every part.
All inputs are finite; a program needn't handle non-finite values.
Results may differ from the reference program's by a relative error of at most 0.001.
Values are sent between devices in bfloat16 or wider.
A program may use at most 1 GiB of HBM per device.

```python
import jax
import jax.numpy as jnp
from jax import lax

GRID_ROWS = 4096
GRID_COLS = 4096
NUM_STEPS = 48
TIME_STEP = 0.5


def block_field(base_key, block_rows, block_cols):
    block_vals = jax.random.normal(base_key, (GRID_ROWS // block_rows, GRID_COLS // block_cols), jnp.float32)
    spread = jnp.broadcast_to(block_vals[:, None, :, None], (GRID_ROWS // block_rows, block_rows, GRID_COLS // block_cols, block_cols))
    return spread.reshape(GRID_ROWS, GRID_COLS)


def setup_inputs(seed: int = 0, part: int = 0) -> dict:
    part_key = jax.random.fold_in(jax.random.key(seed), part)
    key_ublock, key_unoise, key_vblock, key_vnoise = jax.random.split(part_key, 4)
    u_init = block_field(key_ublock, 8, 8) + 0.3 * jax.random.normal(key_unoise, (GRID_ROWS, GRID_COLS), jnp.float32)
    v_init = 0.5 * block_field(key_vblock, 8, 8) + 0.2 * jax.random.normal(key_vnoise, (GRID_ROWS, GRID_COLS), jnp.float32)
    key_pair, key_centre, key_total = jax.random.split(jax.random.key(seed + 1), 3)
    pair_weights = jax.random.uniform(key_pair, (NUM_STEPS, 4), jnp.float32, minval=0.07, maxval=0.13)
    centre = jax.random.uniform(key_centre, (NUM_STEPS,), jnp.float32, minval=0.2, maxval=0.35)
    weight_total = jax.random.uniform(key_total, (NUM_STEPS,), jnp.float32, minval=0.93, maxval=0.98)
    raw_weights = jnp.stack([
        pair_weights[:, 2], pair_weights[:, 0], pair_weights[:, 3],
        pair_weights[:, 1], centre, pair_weights[:, 1],
        pair_weights[:, 3], pair_weights[:, 0], pair_weights[:, 2]], axis=1)
    weight_scale = weight_total / jnp.sum(raw_weights, axis=1)
    stencil_w = (raw_weights * weight_scale[:, None]).reshape(NUM_STEPS, 3, 3)
    return {"u_init": u_init, "v_init": v_init, "stencil_w": stencil_w}


def stencil_sum(field_now, step_w):
    total_acc = step_w[0, 0] * jnp.roll(field_now, (1, 1), axis=(0, 1))
    for tap_index in range(1, 9):
        row_off, col_off = divmod(tap_index, 3)
        total_acc = total_acc + step_w[row_off, col_off] * jnp.roll(field_now, (1 - row_off, 1 - col_off), axis=(0, 1))
    return total_acc


def reference(u_init, v_init, stencil_w):
    def one_step(state_pair, step_w):
        u_now, v_now = state_pair
        v_next = v_now + (stencil_sum(u_now, step_w) - u_now)
        u_next = u_now + TIME_STEP * v_next
        return (u_next, v_next), None

    (u_final, v_final), _ = lax.scan(one_step, (u_init, v_init), stencil_w)
    return (u_final, v_final)
```

```python
import functools

import jax
import jax.numpy as jnp
from jax import lax
from jax.experimental import pallas as pl
from jax.experimental.pallas import tpu as pltpu
from jax.sharding import PartitionSpec as P

LANES = 128
PLANES = 9
HALO = 64
STAGE = 16


def step_weights(w_ref, t):
    return (
        1.5 + 0.5 * w_ref[1, 1, t],
        0.5 * w_ref[0, 0, t],
        0.5 * w_ref[0, 1, t],
        0.5 * w_ref[0, 2, t],
        0.5 * w_ref[1, 0, t],
    )


def chunk(now, old, weights, start, groups):
    centre, w00, w01, w02, w10 = weights

    def taps(g, p):
        return [now[p, pl.ds(start + (8 * g + d), 8), :] for d in (-1, 0, 1)]

    def update(g, p, up, mid, down):
        cols = pl.ds(start + 8 * g, 8)
        new = (
            (centre * mid[1] - old[p, cols, :])
            + w01 * (up[1] + down[1])
            + w10 * (mid[0] + mid[2])
            + w00 * (up[0] + down[2])
            + w02 * (up[2] + down[0])
        )
        old[p, cols, :] = new
        return new

    ghosts = []
    for g in range(groups):
        last = update(g, PLANES, taps(g, PLANES - 1), taps(g, PLANES), taps(g, PLANES + 1))
        first = update(g, 1, taps(g, 0), taps(g, 1), taps(g, 2))
        ghosts.append((pltpu.roll(last, 1, 1), pltpu.roll(first, LANES - 1, 1)))
    for g in range(groups):
        up, mid = taps(g, 1), taps(g, 2)
        for p in range(2, PLANES):
            down = taps(g, p + 1)
            update(g, p, up, mid, down)
            up, mid = mid, down
    for g in range(groups):
        cols = pl.ds(start + 8 * g, 8)
        old[0, cols, :] = ghosts[g][0]
        old[PLANES + 1, cols, :] = ghosts[g][1]


def sweep(now, old, weights, first_col, width):
    first = first_col + HALO
    done = 0
    for groups in (2,):
        cols = 8 * groups
        count = (width - done) // cols
        base = first + done

        def body(i, carry, groups=groups, cols=cols, base=base):
            chunk(now, old, weights, pl.multiple_of(base + i * cols, 8), groups)
            return carry

        lax.fori_loop(0, count, body, 0)
        done = done + count * cols


def kernel(n_row, n_col, steps, u_hbm, v_hbm, w_ref, uo_hbm, vo_hbm, even, odd, u_nat, v_nat, load_sem, store_sem,
           row_send, row_recv, col_send, col_recv):
    rows, cols = u_hbm.shape
    blocks = cols // LANES
    row_id, col_id = lax.axis_index("row"), lax.axis_index("col")
    above, below = lax.rem(row_id + n_row - 1, n_row), lax.rem(row_id + 1, n_row)
    left, right = lax.rem(col_id + n_col - 1, n_col), lax.rem(col_id + 1, n_col)

    def load(f, q):
        src, dst = ((u_hbm, u_nat), (v_hbm, v_nat))[f]
        return pltpu.make_async_copy(
            src.at[:, pl.ds(q * LANES, LANES)], dst.at[q, pl.ds(HALO, rows), :], load_sem.at[f, q])

    def row_copy(f, side, q):
        src, dst = ((u_hbm, u_nat), (v_hbm, v_nat))[f]
        depth = steps
        lines = (rows - depth, 0)[side]
        place = (HALO - depth, HALO + rows)[side]
        return pltpu.make_async_remote_copy(
            src_ref=src.at[pl.ds(lines, depth), pl.ds(q * LANES, LANES)],
            dst_ref=dst.at[q, pl.ds(place, depth), :],
            send_sem=row_send.at[f, side, q], recv_sem=row_recv.at[f, side, q],
            device_id={"row": (below, above)[side]}, device_id_type=pl.DeviceIdType.MESH)

    def col_copy(f, side):
        ref = (even, odd)[f]
        depth = steps
        lines = (HALO + cols - depth, HALO)[side]
        place = (HALO - depth, HALO + cols)[side]
        return pltpu.make_async_remote_copy(
            src_ref=ref.at[:, pl.ds(lines, depth), :], dst_ref=ref.at[:, pl.ds(place, depth), :],
            send_sem=col_send.at[f, side], recv_sem=col_recv.at[f, side],
            device_id={"col": (right, left)[side]}, device_id_type=pl.DeviceIdType.MESH)

    order = [0, blocks - 1] + list(range(1, blocks - 1))
    for q in order:
        for f in (0, 1):
            load(f, q).start()

    barrier = pltpu.get_barrier_semaphore()
    for peer in ({"row": above}, {"row": below}, {"col": left}, {"col": right}):
        pl.semaphore_signal(barrier, inc=1, device_id=peer, device_id_type=pl.DeviceIdType.MESH)
    pl.semaphore_wait(barrier, 4)

    for q in order:
        for f in (0, 1):
            for side in (0, 1):
                row_copy(f, side, q).start()

    for q in order:
        for f in (0, 1):
            load(f, q).wait()
            for side in (0, 1):
                row_copy(f, side, q).wait()

        for s in range(PLANES):
            lines = pl.ds(s, LANES, stride=PLANES)
            u_now = 0.25 * u_nat[q, lines, :]
            u_old = u_now - 0.125 * v_nat[q, lines, :]
            words = pl.ds(HALO + q * LANES, LANES)
            u_now = jnp.transpose(u_now)
            even[s + 1, words, :] = u_now
            odd[s + 1, words, :] = jnp.transpose(u_old)
            if s == 0:
                even[PLANES + 1, words, :] = pltpu.roll(u_now, LANES - 1, 1)
            if s == PLANES - 1:
                even[0, words, :] = pltpu.roll(u_now, 1, 1)

    for f in (0, 1):
        for side in (0, 1):
            col_copy(f, side).start()

    pairs = max(1, min(14, (cols - 160) // 64) // 2)

    def inner_first(t):
        return HALO + STAGE * t

    def outer_first(t):
        return -STAGE * ((steps - 1 - t + STAGE - 1) // STAGE)

    def both(first_pair, last_pair, ranges):
        def body(tt, carry):
            for odd_step, (now, old) in enumerate(((even, odd), (odd, even))):
                t = 2 * tt + odd_step
                ranges(now, old, step_weights(w_ref, t), t)
            return carry

        lax.fori_loop(first_pair, last_pair, body, 0)

    def inner(now, old, weights, t):
        first = inner_first(t)
        sweep(now, old, weights, first, cols - 2 * first)

    def edges(now, old, weights, t):
        first, width = outer_first(t), inner_first(t) - outer_first(t)

        def side(i, carry):
            sweep(now, old, weights, first + i * (cols - first - width - first), width)
            return carry

        lax.fori_loop(0, 2, side, 0)

    def full(now, old, weights, t):
        first = outer_first(t)
        sweep(now, old, weights, first, cols - 2 * first)

    both(0, pairs, inner)
    for f in (0, 1):
        for side in (0, 1):
            col_copy(f, side).wait()
    both(0, pairs, edges)
    both(pairs, steps // 2, full)

    def store(f, q):
        src, dst = ((u_nat, uo_hbm), (v_nat, vo_hbm))[f]
        return pltpu.make_async_copy(
            src.at[q, pl.ds(HALO, rows), :], dst.at[:, pl.ds(q * LANES, LANES)], store_sem.at[f, q])

    for q in range(blocks):
        words = pl.ds(HALO + q * LANES, LANES)
        for s in range(PLANES):
            lines = pl.ds(s, LANES, stride=PLANES)
            u_now = even[s + 1, words, :]
            u_nat[q, lines, :] = jnp.transpose(4.0 * u_now)
            v_nat[q, lines, :] = jnp.transpose(8.0 * (u_now - odd[s + 1, words, :]))
        for f in (0, 1):
            store(f, q).start()
    for q in range(blocks):
        for f in (0, 1):
            store(f, q).wait()


def solution(mesh):
    n_row, n_col = mesh.shape["row"], mesh.shape["col"]
    tile_spec = P(("ens", "row"), "col")

    def local_run(u_tile, v_tile, stencil_w):
        rows, cols = u_tile.shape
        steps = stencil_w.shape[0]
        blocks = cols // LANES
        assert rows + 2 * HALO == LANES * PLANES and steps % 2 == 0 and steps < HALO
        native = pltpu.VMEM((blocks, rows + 2 * HALO, LANES), jnp.float32)
        level = pltpu.VMEM((PLANES + 2, cols + 2 * HALO, LANES), jnp.float32)
        hbm = pl.BlockSpec(memory_space=pl.ANY)
        tile = jax.ShapeDtypeStruct((rows, cols), jnp.float32)
        dma = pltpu.SemaphoreType.DMA
        return pl.pallas_call(
            functools.partial(kernel, n_row, n_col, steps),
            out_shape=(tile, tile),
            in_specs=[hbm, hbm, pl.BlockSpec(memory_space=pltpu.SMEM)],
            out_specs=(hbm, hbm),
            scratch_shapes=[
                level, level, native, native,
                dma((2, blocks)), dma((2, blocks)),
                dma((2, 2, blocks)), dma((2, 2, blocks)), dma((2, 2)), dma((2, 2)),
            ],
            compiler_params=pltpu.CompilerParams(
                collective_id=0, has_side_effects=True, vmem_limit_bytes=56 * 2**20),
            name="wave",
        )(u_tile, v_tile, jnp.transpose(stencil_w, (1, 2, 0)))

    return jax.shard_map(
        local_run, mesh=mesh, in_specs=(tile_spec, tile_spec, P()), out_specs=(tile_spec, tile_spec), check_vma=False)
```

```python
import functools

import jax
import jax.numpy as jnp
from jax import lax
from jax.experimental import pallas as pl
from jax.experimental.pallas import tpu as pltpu
from jax.sharding import PartitionSpec as P

LANES = 128
PLANES = 9
HALO = 64
MARGIN = 128
INNER = 96
STAGE = 16
WIDE = 32
BLOCKS = 4


def step_weights(w_ref, t):
    return (
        1.5 + 0.5 * w_ref[1, 1, t],
        0.5 * w_ref[0, 0, t],
        0.5 * w_ref[0, 1, t],
        0.5 * w_ref[0, 2, t],
        0.5 * w_ref[1, 0, t],
    )


def chunk(now, old, weights, start, blocks, own_ghosts):
    centre, w00, w01, w02, w10 = weights

    def taps(b, p):
        return [now[p, pl.ds(start + (WIDE * b + d), WIDE), :] for d in (-1, 0, 1)]

    def update(b, p, up, mid, down):
        cols = pl.ds(start + WIDE * b, WIDE)
        new = (
            (centre * mid[1] - old[p, cols, :])
            + w01 * (up[1] + down[1])
            + w10 * (mid[0] + mid[2])
            + w00 * (up[0] + down[2])
            + w02 * (up[2] + down[0])
        )
        old[p, cols, :] = new
        return new

    cols = pl.ds(start - WIDE, WIDE)
    ghosts = [(cols, pltpu.roll(old[PLANES, cols, :], 1, 1), pltpu.roll(old[1, cols, :], LANES - 1, 1))]
    for b in range(blocks):
        cols = pl.ds(start + WIDE * b, WIDE)
        last = update(b, PLANES, taps(b, PLANES - 1), taps(b, PLANES), taps(b, PLANES + 1))
        first = update(b, 1, taps(b, 0), taps(b, 1), taps(b, 2))
        if own_ghosts:
            ghosts.append((cols, pltpu.roll(last, 1, 1), pltpu.roll(first, LANES - 1, 1)))
    for b in range(blocks):
        up, mid = taps(b, 1), taps(b, 2)
        for p in range(2, PLANES):
            down = taps(b, p + 1)
            update(b, p, up, mid, down)
            up, mid = mid, down
    for cols, top, bottom in ghosts:
        old[0, cols, :] = top
        old[PLANES + 1, cols, :] = bottom


def sweep(now, old, weights, first_col, width):
    first = first_col + MARGIN
    small, large = WIDE, WIDE * BLOCKS
    few = lax.div(lax.rem(width, large), small)

    def remainder(i, carry):
        chunk(now, old, weights, pl.multiple_of(first + i * small, 8), 1, False)
        return carry

    def body(i, carry):
        chunk(now, old, weights, pl.multiple_of(first + few * small + i * large, 8), BLOCKS, True)
        return carry

    lax.fori_loop(0, few, remainder, 0)
    lax.fori_loop(0, lax.div(width, large), body, 0)


def kernel(n_row, n_col, steps, u_hbm, v_hbm, w_ref, uo_hbm, vo_hbm, even, odd, u_nat, v_nat, load_sem, store_sem,
           row_send, row_recv, col_send, col_recv):
    rows, cols = u_hbm.shape
    blocks = cols // LANES
    row_id, col_id = lax.axis_index("row"), lax.axis_index("col")
    above, below = lax.rem(row_id + n_row - 1, n_row), lax.rem(row_id + 1, n_row)
    left, right = lax.rem(col_id + n_col - 1, n_col), lax.rem(col_id + 1, n_col)

    def load(f, q):
        src, dst = ((u_hbm, u_nat), (v_hbm, v_nat))[f]
        return pltpu.make_async_copy(
            src.at[:, pl.ds(q * LANES, LANES)], dst.at[q, pl.ds(HALO, rows), :], load_sem.at[f, q])

    def row_copy(f, side, q):
        src, dst = ((u_hbm, u_nat), (v_hbm, v_nat))[f]
        depth = steps
        lines = (rows - depth, 0)[side]
        place = (HALO - depth, HALO + rows)[side]
        return pltpu.make_async_remote_copy(
            src_ref=src.at[pl.ds(lines, depth), pl.ds(q * LANES, LANES)],
            dst_ref=dst.at[q, pl.ds(place, depth), :],
            send_sem=row_send.at[f, side, q], recv_sem=row_recv.at[f, side, q],
            device_id={"row": (below, above)[side]}, device_id_type=pl.DeviceIdType.MESH)

    def col_copy(f, side):
        ref, planes = ((even, pl.ds(0, PLANES + 2)), (odd, pl.ds(1, PLANES)))[f]
        depth = steps
        lines = (MARGIN + cols - depth, MARGIN)[side]
        place = (MARGIN - depth, MARGIN + cols)[side]
        return pltpu.make_async_remote_copy(
            src_ref=ref.at[planes, pl.ds(lines, depth), :], dst_ref=ref.at[planes, pl.ds(place, depth), :],
            send_sem=col_send.at[f, side], recv_sem=col_recv.at[f, side],
            device_id={"col": (right, left)[side]}, device_id_type=pl.DeviceIdType.MESH)

    order = [0, blocks - 1] + list(range(1, blocks - 1))
    for q in order:
        for f in (0, 1):
            load(f, q).start()

    barrier = pltpu.get_barrier_semaphore()
    for peer in ({"row": above}, {"row": below}, {"col": left}, {"col": right}):
        pl.semaphore_signal(barrier, inc=1, device_id=peer, device_id_type=pl.DeviceIdType.MESH)
    pl.semaphore_wait(barrier, 4)

    for q in order:
        for f in (0, 1):
            for side in (0, 1):
                row_copy(f, side, q).start()

    for place, q in enumerate(order):
        if place == 3:
            for f in (0, 1):
                for side in (0, 1):
                    col_copy(f, side).start()
        for f in (0, 1):
            load(f, q).wait()
            for side in (0, 1):
                row_copy(f, side, q).wait()

        for s in range(PLANES):
            lines = pl.ds(s, LANES, stride=PLANES)
            u_now = 0.25 * u_nat[q, lines, :]
            u_old = u_now - 0.125 * v_nat[q, lines, :]
            words = pl.ds(MARGIN + q * LANES, LANES)
            u_now = jnp.transpose(u_now)
            even[s + 1, words, :] = u_now
            odd[s + 1, words, :] = jnp.transpose(u_old)
            if s == 0:
                even[PLANES + 1, words, :] = pltpu.roll(u_now, LANES - 1, 1)
            if s == PLANES - 1:
                even[0, words, :] = pltpu.roll(u_now, 1, 1)

    pairs = min(14, (cols - 2 * INNER - 32) // (2 * STAGE)) // 2

    def advance(begin_pair, end_pair, sides, span):
        def pair(v, carry):
            for odd_step, (now, old) in enumerate(((even, odd), (odd, even))):
                t = 2 * v + odd_step
                weights = step_weights(w_ref, t)
                first, width, shift = span(t)

                def side(i, carry, now=now, old=old, first=first, width=width, shift=shift, weights=weights):
                    sweep(now, old, weights, first + i * shift, width)
                    return carry

                lax.fori_loop(0, sides, side, 0)
            return carry

        lax.fori_loop(begin_pair, end_pair, pair, 0)

    def inner(t):
        begin = INNER + STAGE * t
        return begin, cols - 2 * begin, 0

    def edges(t):
        begin = INNER + STAGE * t
        width = WIDE * lax.div(begin + (steps - 1 - t) + WIDE - 1, WIDE)
        return begin - width, width, cols - 2 * begin + width

    def full(t):
        begin = STAGE * lax.div(steps - 1 - t + STAGE - 1, STAGE)
        return -begin, cols + 2 * begin, 0

    advance(0, pairs, 1, inner)
    for f in (0, 1):
        for side in (0, 1):
            col_copy(f, side).wait()
    advance(0, pairs, 2, edges)
    advance(pairs, steps // 2, 1, full)

    def store(f, q):
        src, dst = ((u_nat, uo_hbm), (v_nat, vo_hbm))[f]
        return pltpu.make_async_copy(
            src.at[q, pl.ds(HALO, rows), :], dst.at[:, pl.ds(q * LANES, LANES)], store_sem.at[f, q])

    for q in range(blocks):
        words = pl.ds(MARGIN + q * LANES, LANES)
        for s in range(PLANES):
            lines = pl.ds(s, LANES, stride=PLANES)
            u_now = even[s + 1, words, :]
            u_nat[q, lines, :] = jnp.transpose(4.0 * u_now)
            v_nat[q, lines, :] = jnp.transpose(8.0 * (u_now - odd[s + 1, words, :]))
        for f in (0, 1):
            store(f, q).start()
    for q in range(blocks):
        for f in (0, 1):
            store(f, q).wait()


def solution(mesh):
    n_row, n_col = mesh.shape["row"], mesh.shape["col"]
    tile_spec = P(("ens", "row"), "col")

    def local_run(u_tile, v_tile, stencil_w):
        rows, cols = u_tile.shape
        steps = stencil_w.shape[0]
        blocks = cols // LANES
        assert rows + 2 * HALO == LANES * PLANES and steps % 2 == 0 and steps < HALO
        native = pltpu.VMEM((blocks, rows + 2 * HALO, LANES), jnp.float32)
        level = pltpu.VMEM((PLANES + 2, cols + 2 * MARGIN, LANES), jnp.float32)
        hbm = pl.BlockSpec(memory_space=pl.ANY)
        tile = jax.ShapeDtypeStruct((rows, cols), jnp.float32)
        dma = pltpu.SemaphoreType.DMA
        return pl.pallas_call(
            functools.partial(kernel, n_row, n_col, steps),
            out_shape=(tile, tile),
            in_specs=[hbm, hbm, pl.BlockSpec(memory_space=pltpu.SMEM)],
            out_specs=(hbm, hbm),
            scratch_shapes=[
                level, level, native, native,
                dma((2, blocks)), dma((2, blocks)),
                dma((2, 2, blocks)), dma((2, 2, blocks)), dma((2, 2)), dma((2, 2)),
            ],
            compiler_params=pltpu.CompilerParams(
                collective_id=0, has_side_effects=True, vmem_limit_bytes=56 * 2**20),
            name="wave",
        )(u_tile, v_tile, jnp.transpose(stencil_w, (1, 2, 0)))

    return jax.shard_map(
        local_run, mesh=mesh, in_specs=(tile_spec, tile_spec, P()), out_specs=(tile_spec, tile_spec), check_vma=False)
```

```python
import functools

import jax
import jax.numpy as jnp
from jax import lax
from jax.experimental import pallas as pl
from jax.experimental.pallas import tpu as pltpu
from jax.sharding import PartitionSpec as P

LANES = 128
PLANES = 9
HALO = 64
MARGIN = 128
INNER = 96
STAGE = 16
WIDE = 32
BLOCKS = 4


def step_weights(w_ref, t):
    return (
        1.5 + 0.5 * w_ref[1, 1, t],
        0.5 * w_ref[0, 0, t],
        0.5 * w_ref[0, 1, t],
        0.5 * w_ref[0, 2, t],
        0.5 * w_ref[1, 0, t],
    )


def chunk(now, old, weights, start, blocks, own_ghosts):
    centre, w00, w01, w02, w10 = weights

    def taps(b, p):
        return [now[p, pl.ds(start + (WIDE * b + d), WIDE), :] for d in (-1, 0, 1)]

    def update(b, p, up, mid, down):
        cols = pl.ds(start + WIDE * b, WIDE)
        new = (
            (centre * mid[1] - old[p, cols, :])
            + w01 * (up[1] + down[1])
            + w10 * (mid[0] + mid[2])
            + w00 * (up[0] + down[2])
            + w02 * (up[2] + down[0])
        )
        old[p, cols, :] = new
        return new

    cols = pl.ds(start - WIDE, WIDE)
    ghosts = [(cols, pltpu.roll(old[PLANES, cols, :], 1, 1), pltpu.roll(old[1, cols, :], LANES - 1, 1))]
    for b in range(blocks):
        cols = pl.ds(start + WIDE * b, WIDE)
        last = update(b, PLANES, taps(b, PLANES - 1), taps(b, PLANES), taps(b, PLANES + 1))
        first = update(b, 1, taps(b, 0), taps(b, 1), taps(b, 2))
        if own_ghosts:
            ghosts.append((cols, pltpu.roll(last, 1, 1), pltpu.roll(first, LANES - 1, 1)))
    for b in range(blocks):
        up, mid = taps(b, 1), taps(b, 2)
        for p in range(2, PLANES):
            down = taps(b, p + 1)
            update(b, p, up, mid, down)
            up, mid = mid, down
    for cols, top, bottom in ghosts:
        old[0, cols, :] = top
        old[PLANES + 1, cols, :] = bottom


def sweep(now, old, weights, first_col, width):
    first = first_col + MARGIN
    small, large = WIDE, WIDE * BLOCKS
    few = lax.div(lax.rem(width, large), small)

    def remainder(i, carry):
        chunk(now, old, weights, pl.multiple_of(first + i * small, 8), 1, False)
        return carry

    def body(i, carry):
        chunk(now, old, weights, pl.multiple_of(first + few * small + i * large, 8), BLOCKS, True)
        return carry

    lax.fori_loop(0, few, remainder, 0)
    lax.fori_loop(0, lax.div(width, large), body, 0)


def kernel(n_row, n_col, steps, u_hbm, v_hbm, w_ref, even, odd, u_nat, v_nat, load_sem,
           row_send, row_recv, col_send, col_recv):
    rows, cols = u_hbm.shape
    blocks = cols // LANES
    row_id, col_id = lax.axis_index("row"), lax.axis_index("col")
    above, below = lax.rem(row_id + n_row - 1, n_row), lax.rem(row_id + 1, n_row)
    left, right = lax.rem(col_id + n_col - 1, n_col), lax.rem(col_id + 1, n_col)

    def load(f, q):
        src, dst = ((u_hbm, u_nat), (v_hbm, v_nat))[f]
        return pltpu.make_async_copy(
            src.at[:, pl.ds(q * LANES, LANES)], dst.at[q, pl.ds(HALO, rows), :], load_sem.at[f, q])

    def row_copy(f, side, q):
        src, dst = ((u_hbm, u_nat), (v_hbm, v_nat))[f]
        depth = steps
        lines = (rows - depth, 0)[side]
        place = (HALO - depth, HALO + rows)[side]
        return pltpu.make_async_remote_copy(
            src_ref=src.at[pl.ds(lines, depth), pl.ds(q * LANES, LANES)],
            dst_ref=dst.at[q, pl.ds(place, depth), :],
            send_sem=row_send.at[f, side, q], recv_sem=row_recv.at[f, side, q],
            device_id={"row": (below, above)[side]}, device_id_type=pl.DeviceIdType.MESH)

    def col_copy(f, side):
        ref, planes = ((even, pl.ds(0, PLANES + 2)), (odd, pl.ds(1, PLANES)))[f]
        depth = steps
        lines = (MARGIN + cols - depth, MARGIN)[side]
        place = (MARGIN - depth, MARGIN + cols)[side]
        return pltpu.make_async_remote_copy(
            src_ref=ref.at[planes, pl.ds(lines, depth), :], dst_ref=ref.at[planes, pl.ds(place, depth), :],
            send_sem=col_send.at[f, side], recv_sem=col_recv.at[f, side],
            device_id={"col": (right, left)[side]}, device_id_type=pl.DeviceIdType.MESH)

    order = [0, blocks - 1] + list(range(1, blocks - 1))
    for q in order:
        for f in (0, 1):
            load(f, q).start()

    barrier = pltpu.get_barrier_semaphore()
    for peer in ({"row": above}, {"row": below}, {"col": left}, {"col": right}):
        pl.semaphore_signal(barrier, inc=1, device_id=peer, device_id_type=pl.DeviceIdType.MESH)
    pl.semaphore_wait(barrier, 4)

    for q in order:
        for f in (0, 1):
            for side in (0, 1):
                row_copy(f, side, q).start()

    for place, q in enumerate(order):
        if place == 3:
            for f in (0, 1):
                for side in (0, 1):
                    col_copy(f, side).start()
        for f in (0, 1):
            load(f, q).wait()
            for side in (0, 1):
                row_copy(f, side, q).wait()

        for s in range(PLANES):
            lines = pl.ds(s, LANES, stride=PLANES)
            u_now = 0.25 * u_nat[q, lines, :]
            u_old = u_now - 0.125 * v_nat[q, lines, :]
            words = pl.ds(MARGIN + q * LANES, LANES)
            u_now = jnp.transpose(u_now)
            even[s + 1, words, :] = u_now
            odd[s + 1, words, :] = jnp.transpose(u_old)
            if s == 0:
                even[PLANES + 1, words, :] = pltpu.roll(u_now, LANES - 1, 1)
            if s == PLANES - 1:
                even[0, words, :] = pltpu.roll(u_now, 1, 1)

    pairs = min(14, (cols - 2 * INNER - 32) // (2 * STAGE)) // 2

    def advance(begin_pair, end_pair, sides, span):
        def pair(v, carry):
            for odd_step, (now, old) in enumerate(((even, odd), (odd, even))):
                t = 2 * v + odd_step
                weights = step_weights(w_ref, t)
                first, width, shift = span(t)

                def side(i, carry, now=now, old=old, first=first, width=width, shift=shift, weights=weights):
                    sweep(now, old, weights, first + i * shift, width)
                    return carry

                lax.fori_loop(0, sides, side, 0)
            return carry

        lax.fori_loop(begin_pair, end_pair, pair, 0)

    def inner(t):
        begin = INNER + STAGE * t
        return begin, cols - 2 * begin, 0

    def edges(t):
        begin = INNER + STAGE * t
        width = WIDE * lax.div(begin + (steps - 1 - t) + WIDE - 1, WIDE)
        return begin - width, width, cols - 2 * begin + width

    def full(t):
        begin = STAGE * lax.div(steps - 1 - t + STAGE - 1, STAGE)
        return -begin, cols + 2 * begin, 0

    advance(0, pairs, 1, inner)
    for f in (0, 1):
        for side in (0, 1):
            col_copy(f, side).wait()
    advance(0, pairs, 2, edges)
    advance(pairs, steps // 2, 1, full)


def finish(even, odd, uo_hbm, vo_hbm, u_nat, v_nat, store_sem):
    rows, cols = uo_hbm.shape
    blocks = cols // LANES

    def store(f, q):
        src, dst = ((u_nat, uo_hbm), (v_nat, vo_hbm))[f]
        return pltpu.make_async_copy(
            src.at[q, pl.ds(HALO, rows), :], dst.at[:, pl.ds(q * LANES, LANES)], store_sem.at[f, q])

    for q in range(blocks):
        words = pl.ds(MARGIN + q * LANES, LANES)
        for s in range(PLANES):
            lines = pl.ds(s, LANES, stride=PLANES)
            u_now = even[s + 1, words, :]
            u_nat[q, lines, :] = jnp.transpose(4.0 * u_now)
            v_nat[q, lines, :] = jnp.transpose(8.0 * (u_now - odd[s + 1, words, :]))
        for f in (0, 1):
            store(f, q).start()
    for q in range(blocks):
        for f in (0, 1):
            store(f, q).wait()


def solution(mesh):
    n_row, n_col = mesh.shape["row"], mesh.shape["col"]
    tile_spec = P(("ens", "row"), "col")

    def local_run(u_tile, v_tile, stencil_w):
        rows, cols = u_tile.shape
        steps = stencil_w.shape[0]
        blocks = cols // LANES
        assert rows + 2 * HALO == LANES * PLANES and steps % 2 == 0 and steps < HALO
        native = pltpu.VMEM((blocks, rows + 2 * HALO, LANES), jnp.float32)
        level = jax.ShapeDtypeStruct((PLANES + 2, cols + 2 * MARGIN, LANES), jnp.float32)
        hbm, vmem = pl.BlockSpec(memory_space=pltpu.HBM), pl.BlockSpec(memory_space=pltpu.VMEM)
        tile = jax.ShapeDtypeStruct((rows, cols), jnp.float32)
        dma = pltpu.SemaphoreType.DMA
        levels = pl.pallas_call(
            functools.partial(kernel, n_row, n_col, steps),
            out_shape=(level, level),
            in_specs=[hbm, hbm, pl.BlockSpec(memory_space=pltpu.SMEM)],
            out_specs=(vmem, vmem),
            scratch_shapes=[
                native, native, dma((2, blocks)),
                dma((2, 2, blocks)), dma((2, 2, blocks)), dma((2, 2)), dma((2, 2)),
            ],
            compiler_params=pltpu.CompilerParams(
                collective_id=0, has_side_effects=True, vmem_limit_bytes=26 * 2**20),
            name="wave",
        )(u_tile, v_tile, jnp.transpose(stencil_w, (1, 2, 0)))
        return pl.pallas_call(
            finish,
            out_shape=(tile, tile),
            in_specs=[vmem, vmem],
            out_specs=(hbm, hbm),
            scratch_shapes=[native, native, dma((2, blocks))],
            compiler_params=pltpu.CompilerParams(vmem_limit_bytes=26 * 2**20),
            name="finish",
        )(*levels)

    return jax.shard_map(
        local_run, mesh=mesh, in_specs=(tile_spec, tile_spec, P()), out_specs=(tile_spec, tile_spec), check_vma=False)
```

```python
import functools

import jax
import jax.numpy as jnp
from jax import lax
from jax.experimental import pallas as pl
from jax.experimental.pallas import tpu as pltpu
from jax.sharding import PartitionSpec as P

LANES = 128
PLANES = 9
HALO = 64
MARGIN = 128
INNER = 96
STAGE = 16
WIDE = 32
LAST = 32
BLOCKS = 4


def step_weights(w_ref, t):
    return (
        1.5 + 0.5 * w_ref[1, 1, t],
        0.5 * w_ref[0, 0, t],
        0.5 * w_ref[0, 1, t],
        0.5 * w_ref[0, 2, t],
        0.5 * w_ref[1, 0, t],
    )


def chunk(now, old, weights, start, widths, left_ghosts, own_ghosts):
    centre, w00, w01, w02, w10 = weights
    blocks = [(sum(widths[:i]), width) for i, width in enumerate(widths)]

    def taps(block, p):
        return [now[p, pl.ds(start + (block[0] + d), block[1]), :] for d in (-1, 0, 1)]

    def update(block, p, up, mid, down):
        cols = pl.ds(start + block[0], block[1])
        new = (
            (centre * mid[1] - old[p, cols, :])
            + w01 * (up[1] + down[1])
            + w10 * (mid[0] + mid[2])
            + w00 * (up[0] + down[2])
            + w02 * (up[2] + down[0])
        )
        old[p, cols, :] = new
        return new

    ghosts = []
    if left_ghosts:
        cols = pl.ds(start - WIDE, WIDE)
        ghosts.append((cols, pltpu.roll(old[PLANES, cols, :], 1, 1), pltpu.roll(old[1, cols, :], LANES - 1, 1)))
    for b in blocks:
        cols = pl.ds(start + b[0], b[1])
        last = update(b, PLANES, taps(b, PLANES - 1), taps(b, PLANES), taps(b, PLANES + 1))
        first = update(b, 1, taps(b, 0), taps(b, 1), taps(b, 2))
        if own_ghosts:
            ghosts.append((cols, pltpu.roll(last, 1, 1), pltpu.roll(first, LANES - 1, 1)))
    for b in blocks:
        up, mid = taps(b, 1), taps(b, 2)
        for p in range(2, PLANES):
            down = taps(b, p + 1)
            update(b, p, up, mid, down)
            up, mid = mid, down
    for cols, top, bottom in ghosts:
        old[0, cols, :] = top
        old[PLANES + 1, cols, :] = bottom


def sweep(now, old, weights, first_col, width):
    first = first_col + MARGIN
    small, large = WIDE, WIDE * BLOCKS
    few = lax.div(lax.rem(width, large), small)

    def remainder(i, carry):
        chunk(now, old, weights, pl.multiple_of(first + i * small, 8), [WIDE], True, False)
        return carry

    def body(i, carry):
        chunk(now, old, weights, pl.multiple_of(first + few * small + i * large, 8), [WIDE] * BLOCKS, True, True)
        return carry

    lax.fori_loop(0, few, remainder, 0)
    lax.fori_loop(0, lax.div(width, large), body, 0)


def wide_sweep(now, old, weights, cols):
    part = (cols + 2 * LAST) // 4
    widths = [WIDE] * (part // WIDE - 1)
    widths.append(part - sum(widths))

    def body(i, carry):
        chunk(now, old, weights, pl.multiple_of(MARGIN - LAST + i * part, 8), widths, False, True)
        return carry

    lax.fori_loop(0, 4, body, 0)


def kernel(n_row, n_col, steps, u_hbm, v_hbm, w_hbm, even, odd, u_nat, v_nat, w_ref, load_sem, w_sem,
           row_send, row_recv, col_send, col_recv):
    rows, cols = u_hbm.shape
    blocks = cols // LANES
    row_id, col_id = lax.axis_index("row"), lax.axis_index("col")
    above, below = lax.rem(row_id + n_row - 1, n_row), lax.rem(row_id + 1, n_row)
    left, right = lax.rem(col_id + n_col - 1, n_col), lax.rem(col_id + 1, n_col)

    def load(f, q):
        src, dst = ((u_hbm, u_nat), (v_hbm, v_nat))[f]
        return pltpu.make_async_copy(
            src.at[:, pl.ds(q * LANES, LANES)], dst.at[q, pl.ds(HALO, rows), :], load_sem.at[f, q])

    def row_copy(f, side, q):
        ref = (u_nat, v_nat)[f]
        depth = steps
        lines = (HALO + rows - depth, HALO)[side]
        place = (HALO - depth, HALO + rows)[side]
        return pltpu.make_async_remote_copy(
            src_ref=ref.at[q, pl.ds(lines, depth), :], dst_ref=ref.at[q, pl.ds(place, depth), :],
            send_sem=row_send.at[f, side, q], recv_sem=row_recv.at[f, side, q],
            device_id={"row": (below, above)[side]}, device_id_type=pl.DeviceIdType.MESH)

    def col_copy(f, side):
        ref, planes = (even, odd)[f], pl.ds(1, PLANES)
        depth = steps
        lines = (MARGIN + cols - depth, MARGIN)[side]
        place = (MARGIN - depth, MARGIN + cols)[side]
        return pltpu.make_async_remote_copy(
            src_ref=ref.at[planes, pl.ds(lines, depth), :], dst_ref=ref.at[planes, pl.ds(place, depth), :],
            send_sem=col_send.at[f, side], recv_sem=col_recv.at[f, side],
            device_id={"col": (right, left)[side]}, device_id_type=pl.DeviceIdType.MESH)

    load_weights = pltpu.make_async_copy(w_hbm, w_ref, w_sem)
    load_weights.start()
    order = [0, blocks - 1] + list(range(1, blocks - 1))
    for q in order:
        for f in (0, 1):
            load(f, q).start()

    barrier = pltpu.get_barrier_semaphore()
    for peer in ({"row": above}, {"row": below}, {"col": left}, {"col": right}):
        pl.semaphore_signal(barrier, inc=1, device_id=peer, device_id_type=pl.DeviceIdType.MESH)
    pl.semaphore_wait(barrier, 4)

    for q in order:
        for f in (0, 1):
            load(f, q).wait()
            for side in (0, 1):
                row_copy(f, side, q).start()

    for place, q in enumerate(order):
        if place == 3:
            for f in (0, 1):
                for side in (0, 1):
                    col_copy(f, side).start()
        for f in (0, 1):
            for side in (0, 1):
                row_copy(f, side, q).wait()

        for s in range(PLANES):
            lines = pl.ds(s, LANES, stride=PLANES)
            u_now = 0.25 * u_nat[q, lines, :]
            u_old = u_now - 0.125 * v_nat[q, lines, :]
            words = pl.ds(MARGIN + q * LANES, LANES)
            u_now = jnp.transpose(u_now)
            even[s + 1, words, :] = u_now
            odd[s + 1, words, :] = jnp.transpose(u_old)
            if s == 0:
                even[PLANES + 1, words, :] = pltpu.roll(u_now, LANES - 1, 1)
            if s == PLANES - 1:
                even[0, words, :] = pltpu.roll(u_now, 1, 1)

    pairs = min(8, steps // 4, (cols - 2 * INNER - 128) // (4 * STAGE))
    assert steps - 2 * pairs <= LAST + 1

    def advance(begin_pair, end_pair, step):
        def pair(v, carry):
            for odd_step, (now, old) in enumerate(((even, odd), (odd, even))):
                t = 2 * v + odd_step
                step(now, old, step_weights(w_ref, t), t)
            return carry

        lax.fori_loop(begin_pair, end_pair, pair, 0)

    def inner(now, old, weights, t):
        begin = INNER + STAGE * t
        sweep(now, old, weights, begin, cols - 2 * begin)

    def edges(now, old, weights, t):
        begin = INNER + STAGE * t
        width = WIDE * lax.div(begin + (steps - 1 - t) + WIDE - 1, WIDE)

        def side(i, carry):
            sweep(now, old, weights, begin - width + i * (cols - 2 * begin + width), width)
            return carry

        lax.fori_loop(0, 2, side, 0)

    def full(now, old, weights, t):
        wide_sweep(now, old, weights, cols)

    load_weights.wait()
    advance(0, pairs, inner)
    for f in (0, 1):
        for side in (0, 1):
            col_copy(f, side).wait()
    for place in (MARGIN - steps, MARGIN + cols):
        words = pl.ds(place, steps)
        even[0, words, :] = pltpu.roll(even[PLANES, words, :], 1, 1)
        even[PLANES + 1, words, :] = pltpu.roll(even[1, words, :], LANES - 1, 1)
    advance(0, pairs, edges)
    advance(pairs, steps // 2, full)


def finish(even, odd, uo_hbm, vo_hbm, u_nat, v_nat, store_sem):
    rows, cols = uo_hbm.shape
    blocks = cols // LANES

    def store(f, q):
        src, dst = ((u_nat, uo_hbm), (v_nat, vo_hbm))[f]
        return pltpu.make_async_copy(
            src.at[q, pl.ds(HALO, rows), :], dst.at[:, pl.ds(q * LANES, LANES)], store_sem.at[f, q])

    for q in range(blocks):
        words = pl.ds(MARGIN + q * LANES, LANES)
        for s in range(PLANES):
            lines = pl.ds(s, LANES, stride=PLANES)
            u_now = even[s + 1, words, :]
            u_nat[q, lines, :] = jnp.transpose(4.0 * u_now)
            v_nat[q, lines, :] = jnp.transpose(8.0 * (u_now - odd[s + 1, words, :]))
        for f in (0, 1):
            store(f, q).start()
    for q in range(blocks):
        for f in (0, 1):
            store(f, q).wait()


def solution(mesh):
    n_row, n_col = mesh.shape["row"], mesh.shape["col"]
    tile_spec = P(("ens", "row"), "col")

    def local_run(u_tile, v_tile, stencil_w):
        rows, cols = u_tile.shape
        steps = stencil_w.shape[0]
        blocks = cols // LANES
        assert rows + 2 * HALO == LANES * PLANES and steps % 2 == 0 and steps < HALO
        native = pltpu.VMEM((blocks, rows + 2 * HALO, LANES), jnp.float32)
        level = jax.ShapeDtypeStruct((PLANES + 2, cols + 2 * MARGIN, LANES), jnp.float32)
        hbm, vmem = pl.BlockSpec(memory_space=pltpu.HBM), pl.BlockSpec(memory_space=pltpu.VMEM)
        tile = jax.ShapeDtypeStruct((rows, cols), jnp.float32)
        dma = pltpu.SemaphoreType.DMA
        levels = pl.pallas_call(
            functools.partial(kernel, n_row, n_col, steps),
            out_shape=(level, level),
            in_specs=[hbm, hbm, hbm],
            out_specs=(vmem, vmem),
            scratch_shapes=[
                native, native, pltpu.SMEM((3, 3, steps), jnp.float32), dma((2, blocks)), dma(()),
                dma((2, 2, blocks)), dma((2, 2, blocks)), dma((2, 2)), dma((2, 2)),
            ],
            compiler_params=pltpu.CompilerParams(
                collective_id=0, has_side_effects=True, vmem_limit_bytes=26 * 2**20),
            name="wave",
        )(*(pltpu.with_memory_space_constraint(x, pltpu.HBM) for x in (u_tile, v_tile, jnp.transpose(stencil_w, (1, 2, 0)))))
        return pl.pallas_call(
            finish,
            out_shape=(tile, tile),
            in_specs=[vmem, vmem],
            out_specs=(hbm, hbm),
            scratch_shapes=[native, native, dma((2, blocks))],
            compiler_params=pltpu.CompilerParams(vmem_limit_bytes=26 * 2**20),
            name="finish",
        )(*levels)

    return jax.shard_map(
        local_run, mesh=mesh, in_specs=(tile_spec, tile_spec, P()), out_specs=(tile_spec, tile_spec), check_vma=False)
```

```python
import functools

import jax
import jax.numpy as jnp
from jax import lax
from jax.experimental import pallas as pl
from jax.experimental.pallas import tpu as pltpu
from jax.sharding import PartitionSpec as P

LANES = 128
PLANES = 9
HALO = 64
MARGIN = 128
INNER = 96
STAGE = 16
WIDE = 32
PARTS = 2
BLOCKS = 4
TAPS = 5


def step_weights(w_ref, t):
    return (
        1.5 + 0.5 * w_ref[1, 1, t],
        0.5 * w_ref[0, 0, t],
        0.5 * w_ref[0, 1, t],
        0.5 * w_ref[0, 2, t],
        0.5 * w_ref[1, 0, t],
    )


def chunk(now, old, weights, start, widths, left_ghosts, own_ghosts):
    centre, w00, w01, w02, w10 = weights
    blocks = [(sum(widths[:i]), width) for i, width in enumerate(widths)]

    def taps(block, p):
        return [now[p, pl.ds(start + (block[0] + d), block[1]), :] for d in (-1, 0, 1)]

    def update(block, p, up, mid, down):
        cols = pl.ds(start + block[0], block[1])
        new = (
            (centre * mid[1] - old[p, cols, :])
            + w01 * (up[1] + down[1])
            + w10 * (mid[0] + mid[2])
            + w00 * (up[0] + down[2])
            + w02 * (up[2] + down[0])
        )
        old[p, cols, :] = new
        return new

    ghosts = []
    if left_ghosts:
        cols = pl.ds(start - WIDE, WIDE)
        ghosts.append((cols, pltpu.roll(old[PLANES, cols, :], 1, 1), pltpu.roll(old[1, cols, :], LANES - 1, 1)))
    for b in blocks:
        cols = pl.ds(start + b[0], b[1])
        last = update(b, PLANES, taps(b, PLANES - 1), taps(b, PLANES), taps(b, PLANES + 1))
        first = update(b, 1, taps(b, 0), taps(b, 1), taps(b, 2))
        if own_ghosts:
            ghosts.append((cols, pltpu.roll(last, 1, 1), pltpu.roll(first, LANES - 1, 1)))
    for b in blocks:
        up, mid = taps(b, 1), taps(b, 2)
        for p in range(2, PLANES):
            down = taps(b, p + 1)
            update(b, p, up, mid, down)
            up, mid = mid, down
    for cols, top, bottom in ghosts:
        old[0, cols, :] = top
        old[PLANES + 1, cols, :] = bottom


def sweep(now, old, weights, first_col, width):
    first = first_col + MARGIN
    small, large = WIDE, WIDE * BLOCKS
    few = lax.div(lax.rem(width, large), small)

    def remainder(i, carry):
        chunk(now, old, weights, pl.multiple_of(first + i * small, 8), [WIDE], True, False)
        return carry

    def body(i, carry):
        chunk(now, old, weights, pl.multiple_of(first + few * small + i * large, 8), [WIDE] * BLOCKS, True, True)
        return carry

    lax.fori_loop(0, few, remainder, 0)
    lax.fori_loop(0, lax.div(width, large), body, 0)


def wide_sweep(now, old, weights, cols, extra):
    part = (cols + 2 * extra) // PARTS
    widths = [WIDE] * (part // WIDE - 1)
    widths.append(part - sum(widths))

    def body(i, carry):
        chunk(now, old, weights, pl.multiple_of(MARGIN - extra + i * part, 8), widths, False, True)
        return carry

    lax.fori_loop(0, PARTS, body, 0)


def start(n_row, n_col, steps, pairs, u_hbm, v_hbm, w_hbm, even, odd, w_rows, u_nat, v_nat, w_ref, load_sem, w_sem,
           row_send, row_recv, col_send, col_recv):
    rows, cols = u_hbm.shape
    blocks = cols // LANES
    row_id, col_id = lax.axis_index("row"), lax.axis_index("col")
    above, below = lax.rem(row_id + n_row - 1, n_row), lax.rem(row_id + 1, n_row)
    left, right = lax.rem(col_id + n_col - 1, n_col), lax.rem(col_id + 1, n_col)

    def load(f, q):
        src, dst = ((u_hbm, u_nat), (v_hbm, v_nat))[f]
        return pltpu.make_async_copy(
            src.at[:, pl.ds(q * LANES, LANES)], dst.at[q, pl.ds(HALO, rows), :], load_sem.at[f, q])

    def row_copy(f, side, q):
        ref = (u_nat, v_nat)[f]
        depth = steps
        lines = (HALO + rows - depth, HALO)[side]
        place = (HALO - depth, HALO + rows)[side]
        return pltpu.make_async_remote_copy(
            src_ref=ref.at[q, pl.ds(lines, depth), :], dst_ref=ref.at[q, pl.ds(place, depth), :],
            send_sem=row_send.at[f, side, q], recv_sem=row_recv.at[f, side, q],
            device_id={"row": (below, above)[side]}, device_id_type=pl.DeviceIdType.MESH)

    def col_copy(f, side):
        ref, planes = (even, odd)[f], pl.ds(1, PLANES)
        depth = steps
        lines = (MARGIN + cols - depth, MARGIN)[side]
        place = (MARGIN - depth, MARGIN + cols)[side]
        return pltpu.make_async_remote_copy(
            src_ref=ref.at[planes, pl.ds(lines, depth), :], dst_ref=ref.at[planes, pl.ds(place, depth), :],
            send_sem=col_send.at[f, side], recv_sem=col_recv.at[f, side],
            device_id={"col": (right, left)[side]}, device_id_type=pl.DeviceIdType.MESH)

    load_weights = pltpu.make_async_copy(w_hbm, w_ref, w_sem)
    load_weights.start()
    order = [0, blocks - 1] + list(range(1, blocks - 1))
    for q in order:
        for f in (0, 1):
            load(f, q).start()

    barrier = pltpu.get_barrier_semaphore()
    for peer in ({"row": above}, {"row": below}, {"col": left}, {"col": right}):
        pl.semaphore_signal(barrier, inc=1, device_id=peer, device_id_type=pl.DeviceIdType.MESH)
    pl.semaphore_wait(barrier, 4)

    for q in order:
        for f in (0, 1):
            load(f, q).wait()
            for side in (0, 1):
                row_copy(f, side, q).start()

    load_weights.wait()

    def spread(t, carry):
        for k, weight in enumerate(step_weights(w_ref, t)):
            w_rows[t, pl.ds(k, 1), :] = jnp.full((1, LANES), weight, jnp.float32)
        return carry

    lax.fori_loop(0, steps, spread, 0)

    for place, q in enumerate(order):
        if place == 3:
            for f in (0, 1):
                for side in (0, 1):
                    col_copy(f, side).start()
        for f in (0, 1):
            for side in (0, 1):
                row_copy(f, side, q).wait()

        for s in range(PLANES):
            lines = pl.ds(s, LANES, stride=PLANES)
            u_now = 0.25 * u_nat[q, lines, :]
            u_old = u_now - 0.125 * v_nat[q, lines, :]
            words = pl.ds(MARGIN + q * LANES, LANES)
            u_now = jnp.transpose(u_now)
            even[s + 1, words, :] = u_now
            odd[s + 1, words, :] = jnp.transpose(u_old)
            if s == 0:
                even[PLANES + 1, words, :] = pltpu.roll(u_now, LANES - 1, 1)
            if s == PLANES - 1:
                even[0, words, :] = pltpu.roll(u_now, 1, 1)

    def advance(step):
        def pair(v, carry):
            for odd_step, (now, old) in enumerate(((even, odd), (odd, even))):
                t = 2 * v + odd_step
                step(now, old, step_weights(w_ref, t), t)
            return carry

        lax.fori_loop(0, pairs, pair, 0)

    def inner(now, old, weights, t):
        begin = INNER + STAGE * t
        sweep(now, old, weights, begin, cols - 2 * begin)

    def edges(now, old, weights, t):
        begin = INNER + STAGE * t
        width = WIDE * lax.div(begin + (steps - 1 - t) + WIDE - 1, WIDE)

        def side(i, carry):
            sweep(now, old, weights, begin - width + i * (cols - 2 * begin + width), width)
            return carry

        lax.fori_loop(0, 2, side, 0)

    advance(inner)
    for f in (0, 1):
        for side in (0, 1):
            col_copy(f, side).wait()
    for place in (MARGIN - steps, MARGIN + cols):
        words = pl.ds(place, steps)
        even[0, words, :] = pltpu.roll(even[PLANES, words, :], 1, 1)
        even[PLANES + 1, words, :] = pltpu.roll(even[1, words, :], LANES - 1, 1)
    advance(edges)


def finish(steps, begin, even_in, odd_in, w_rows, uo_hbm, vo_hbm, even, odd, u_nat, v_nat, store_sem):
    del even_in, odd_in
    rows, cols = uo_hbm.shape
    blocks = cols // LANES

    def weights_of(t):
        return [w_rows[t, pl.ds(k, 1), :] for k in range(TAPS)]

    def pair(v, carry, extra):
        for odd_step, (now, old) in enumerate(((even, odd), (odd, even))):
            wide_sweep(now, old, weights_of(2 * v + odd_step), cols, extra)
        return carry

    t = begin
    while steps - t > 2:
        extra = 8 * ((steps - 1 - t + 7) // 8)
        until = min(steps - 2, steps - 1 - (extra - 8))
        until += until % 2
        until = min(until, steps - 2)
        lax.fori_loop(t // 2, until // 2, functools.partial(pair, extra=extra), 0)
        t = until
    wide_sweep(even, odd, weights_of(steps - 2), cols, 8)

    last = weights_of(steps - 1)

    def store(f, q):
        src, dst = ((u_nat, uo_hbm), (v_nat, vo_hbm))[f]
        return pltpu.make_async_copy(
            src.at[q, pl.ds(HALO, rows), :],
            dst.at[:, pl.ds(pl.multiple_of(q * LANES, LANES), LANES)], store_sem.at[f, q])

    def step(q):
        chunk(odd, even, last, pl.multiple_of(MARGIN + q * LANES, LANES), [WIDE] * (LANES // WIDE), False, False)

    def write(q):
        words = pl.ds(pl.multiple_of(MARGIN + q * LANES, LANES), LANES)
        for s in range(PLANES):
            lines = pl.ds(s, LANES, stride=PLANES)
            u_now = even[s + 1, words, :]
            u_nat[q, lines, :] = jnp.transpose(4.0 * u_now)
            v_nat[q, lines, :] = jnp.transpose(8.0 * (u_now - odd[s + 1, words, :]))
        for f in (0, 1):
            store(f, q).start()

    def both(q, carry):
        step(q)
        write(q - 1)
        return carry

    step(0)
    lax.fori_loop(1, blocks, both, 0)
    write(blocks - 1)
    for q in range(blocks):
        for f in (0, 1):
            store(f, q).wait()


def solution(mesh):
    n_row, n_col = mesh.shape["row"], mesh.shape["col"]
    tile_spec = P(("ens", "row"), "col")

    def local_run(u_tile, v_tile, stencil_w):
        rows, cols = u_tile.shape
        steps = stencil_w.shape[0]
        blocks = cols // LANES
        assert rows + 2 * HALO == LANES * PLANES and steps % 2 == 0 and steps < HALO
        native = pltpu.VMEM((blocks, rows + 2 * HALO, LANES), jnp.float32)
        level = jax.ShapeDtypeStruct((PLANES + 2, cols + 2 * MARGIN, LANES), jnp.float32)
        hbm, vmem = pl.BlockSpec(memory_space=pltpu.HBM), pl.BlockSpec(memory_space=pltpu.VMEM)
        tile = jax.ShapeDtypeStruct((rows, cols), jnp.float32)
        dma = pltpu.SemaphoreType.DMA
        pairs = min(8, steps // 4, (cols - 2 * INNER - 128) // (4 * STAGE))
        w_rows = jax.ShapeDtypeStruct((steps, 8, LANES), jnp.float32)
        state = pl.pallas_call(
            functools.partial(start, n_row, n_col, steps, pairs),
            out_shape=(level, level, w_rows),
            in_specs=[hbm, hbm, hbm],
            out_specs=(vmem, vmem, vmem),
            scratch_shapes=[
                native, native, pltpu.SMEM((3, 3, steps), jnp.float32), dma((2, blocks)), dma(()),
                dma((2, 2, blocks)), dma((2, 2, blocks)), dma((2, 2)), dma((2, 2)),
            ],
            compiler_params=pltpu.CompilerParams(
                collective_id=0, has_side_effects=True, vmem_limit_bytes=26 * 2**20),
            name="start",
        )(*(pltpu.with_memory_space_constraint(x, pltpu.HBM) for x in (u_tile, v_tile, jnp.transpose(stencil_w, (1, 2, 0)))))
        return pl.pallas_call(
            functools.partial(finish, steps, 2 * pairs),
            out_shape=(tile, tile, level, level),
            in_specs=[vmem, vmem, vmem],
            out_specs=(hbm, hbm, vmem, vmem),
            input_output_aliases={0: 2, 1: 3},
            scratch_shapes=[native, native, dma((2, blocks))],
            compiler_params=pltpu.CompilerParams(vmem_limit_bytes=26 * 2**20),
            name="finish",
        )(*state)[:2]

    return jax.shard_map(
        local_run, mesh=mesh, in_specs=(tile_spec, tile_spec, P()), out_specs=(tile_spec, tile_spec), check_vma=False)
```

```python
import functools

import jax
import jax.numpy as jnp
from jax import lax
from jax.experimental import pallas as pl
from jax.experimental.pallas import tpu as pltpu
from jax.sharding import PartitionSpec as P

LANES = 128
PLANES = 9
HALO = 64
MARGIN = 128
INNER = 96
STAGE = 16
WIDE = 32
PARTS = 2
BLOCKS = 4
TAPS = 5


def step_weights(w_ref, t):
    return (
        1.5 + 0.5 * w_ref[1, 1, t],
        0.5 * w_ref[0, 0, t],
        0.5 * w_ref[0, 1, t],
        0.5 * w_ref[0, 2, t],
        0.5 * w_ref[1, 0, t],
    )


def chunk(now, old, weights, start, widths, left_ghosts, own_ghosts):
    centre, w00, w01, w02, w10 = weights
    blocks = [(sum(widths[:i]), width) for i, width in enumerate(widths)]

    def taps(block, p):
        return [now[p, pl.ds(start + (block[0] + d), block[1]), :] for d in (-1, 0, 1)]

    def update(block, p, up, mid, down):
        cols = pl.ds(start + block[0], block[1])
        new = (
            (centre * mid[1] - old[p, cols, :])
            + w01 * (up[1] + down[1])
            + w10 * (mid[0] + mid[2])
            + w00 * (up[0] + down[2])
            + w02 * (up[2] + down[0])
        )
        old[p, cols, :] = new
        return new

    ghosts = []
    if left_ghosts:
        cols = pl.ds(start - WIDE, WIDE)
        ghosts.append((cols, pltpu.roll(old[PLANES, cols, :], 1, 1), pltpu.roll(old[1, cols, :], LANES - 1, 1)))
    for b in blocks:
        cols = pl.ds(start + b[0], b[1])
        last = update(b, PLANES, taps(b, PLANES - 1), taps(b, PLANES), taps(b, PLANES + 1))
        first = update(b, 1, taps(b, 0), taps(b, 1), taps(b, 2))
        if own_ghosts:
            ghosts.append((cols, pltpu.roll(last, 1, 1), pltpu.roll(first, LANES - 1, 1)))
    for b in blocks:
        up, mid = taps(b, 1), taps(b, 2)
        for p in range(2, PLANES):
            down = taps(b, p + 1)
            update(b, p, up, mid, down)
            up, mid = mid, down
    for cols, top, bottom in ghosts:
        old[0, cols, :] = top
        old[PLANES + 1, cols, :] = bottom


def sweep(now, old, weights, first_col, width):
    first = first_col + MARGIN
    small, large = WIDE, WIDE * BLOCKS
    few = lax.div(lax.rem(width, large), small)

    def remainder(i, carry):
        chunk(now, old, weights, pl.multiple_of(first + i * small, 8), [WIDE], True, False)
        return carry

    def body(i, carry):
        chunk(now, old, weights, pl.multiple_of(first + few * small + i * large, 8), [WIDE] * BLOCKS, True, True)
        return carry

    lax.fori_loop(0, few, remainder, 0)
    lax.fori_loop(0, lax.div(width, large), body, 0)


def wide_sweep(now, old, weights, cols, extra):
    part = (cols + 2 * extra) // PARTS
    widths = [WIDE] * (part // WIDE - 1)
    widths.append(part - sum(widths))

    def body(i, carry):
        chunk(now, old, weights, pl.multiple_of(MARGIN - extra + i * part, 8), widths, False, True)
        return carry

    lax.fori_loop(0, PARTS, body, 0)


def start(n_row, n_col, steps, pairs, u_hbm, v_hbm, w_hbm, even, odd, w_rows, u_nat, v_nat, w_ref, load_sem, w_sem,
           row_send, row_recv, col_send, col_recv):
    rows, cols = u_hbm.shape
    blocks = cols // LANES
    row_id, col_id = lax.axis_index("row"), lax.axis_index("col")
    above, below = lax.rem(row_id + n_row - 1, n_row), lax.rem(row_id + 1, n_row)
    left, right = lax.rem(col_id + n_col - 1, n_col), lax.rem(col_id + 1, n_col)

    def load(f, q):
        src, dst = ((u_hbm, u_nat), (v_hbm, v_nat))[f]
        return pltpu.make_async_copy(
            src.at[:, pl.ds(q * LANES, LANES)], dst.at[q, pl.ds(HALO, rows), :], load_sem.at[f, q])

    def row_copy(f, side, q):
        ref = (u_nat, v_nat)[f]
        depth = steps
        lines = (HALO + rows - depth, HALO)[side]
        place = (HALO - depth, HALO + rows)[side]
        return pltpu.make_async_remote_copy(
            src_ref=ref.at[q, pl.ds(lines, depth), :], dst_ref=ref.at[q, pl.ds(place, depth), :],
            send_sem=row_send.at[f, side, q], recv_sem=row_recv.at[f, side, q],
            device_id={"row": (below, above)[side]}, device_id_type=pl.DeviceIdType.MESH)

    def col_copy(f, side):
        ref, planes = (even, odd)[f], pl.ds(1, PLANES)
        depth = steps
        lines = (MARGIN + cols - depth, MARGIN)[side]
        place = (MARGIN - depth, MARGIN + cols)[side]
        return pltpu.make_async_remote_copy(
            src_ref=ref.at[planes, pl.ds(lines, depth), :], dst_ref=ref.at[planes, pl.ds(place, depth), :],
            send_sem=col_send.at[f, side], recv_sem=col_recv.at[f, side],
            device_id={"col": (right, left)[side]}, device_id_type=pl.DeviceIdType.MESH)

    load_weights = pltpu.make_async_copy(w_hbm, w_ref, w_sem)
    load_weights.start()
    order = [0, blocks - 1] + list(range(1, blocks - 1))
    for q in order:
        for f in (0, 1):
            load(f, q).start()

    barrier = pltpu.get_barrier_semaphore()
    for peer in ({"row": above}, {"row": below}, {"col": left}, {"col": right}):
        pl.semaphore_signal(barrier, inc=1, device_id=peer, device_id_type=pl.DeviceIdType.MESH)
    pl.semaphore_wait(barrier, 4)

    for q in order:
        for f in (0, 1):
            load(f, q).wait()
            for side in (0, 1):
                row_copy(f, side, q).start()

    load_weights.wait()

    def spread(t, carry):
        for k, weight in enumerate(step_weights(w_ref, t)):
            w_rows[t, pl.ds(k, 1), :] = jnp.full((1, LANES), weight, jnp.float32)
        return carry

    lax.fori_loop(0, steps, spread, 0)

    for place, q in enumerate(order):
        if place == 3:
            for f in (0, 1):
                for side in (0, 1):
                    col_copy(f, side).start()
        for f in (0, 1):
            for side in (0, 1):
                row_copy(f, side, q).wait()

        for s in range(PLANES):
            lines = pl.ds(s, LANES, stride=PLANES)
            u_now = 0.25 * u_nat[q, lines, :]
            u_old = u_now - 0.125 * v_nat[q, lines, :]
            words = pl.ds(MARGIN + q * LANES, LANES)
            u_now = jnp.transpose(u_now)
            even[s + 1, words, :] = u_now
            odd[s + 1, words, :] = jnp.transpose(u_old)
            if s == 0:
                even[PLANES + 1, words, :] = pltpu.roll(u_now, LANES - 1, 1)
            if s == PLANES - 1:
                even[0, words, :] = pltpu.roll(u_now, 1, 1)

    def advance(step):
        def pair(v, carry):
            for odd_step, (now, old) in enumerate(((even, odd), (odd, even))):
                t = 2 * v + odd_step
                step(now, old, step_weights(w_ref, t), t)
            return carry

        lax.fori_loop(0, pairs, pair, 0)

    def inner(now, old, weights, t):
        begin = INNER + STAGE * t
        sweep(now, old, weights, begin, cols - 2 * begin)

    def edges(now, old, weights, t):
        begin = INNER + STAGE * t
        width = WIDE * lax.div(begin + (steps - 1 - t) + WIDE - 1, WIDE)

        def side(i, carry):
            sweep(now, old, weights, begin - width + i * (cols - 2 * begin + width), width)
            return carry

        lax.fori_loop(0, 2, side, 0)

    advance(inner)
    for f in (0, 1):
        for side in (0, 1):
            col_copy(f, side).wait()
    for place in (MARGIN - steps, MARGIN + cols):
        words = pl.ds(place, steps)
        even[0, words, :] = pltpu.roll(even[PLANES, words, :], 1, 1)
        even[PLANES + 1, words, :] = pltpu.roll(even[1, words, :], LANES - 1, 1)
    advance(edges)


def finish(steps, begin, even_in, odd_in, w_rows, uo_hbm, vo_hbm, even, odd, u_nat, v_nat, store_sem):
    del even_in, odd_in
    rows, cols = uo_hbm.shape
    blocks = cols // LANES

    def weights_of(t):
        return [w_rows[t, pl.ds(k, 1), :] for k in range(TAPS)]

    def pair(v, carry, extra):
        for odd_step, (now, old) in enumerate(((even, odd), (odd, even))):
            wide_sweep(now, old, weights_of(2 * v + odd_step), cols, extra)
        return carry

    t = begin
    while steps - t > 2:
        extra = 8 * ((steps - 1 - t + 7) // 8)
        until = min(steps - 2, steps - 1 - (extra - 8))
        until += until % 2
        until = min(until, steps - 2)
        lax.fori_loop(t // 2, until // 2, functools.partial(pair, extra=extra), 0)
        t = until
    wide_sweep(even, odd, weights_of(steps - 2), cols, 8)

    last = weights_of(steps - 1)

    def store(f, q):
        src, dst = ((u_nat, uo_hbm), (v_nat, vo_hbm))[f]
        return pltpu.make_async_copy(
            src.at[q, pl.ds(HALO, rows), :],
            dst.at[:, pl.ds(q * LANES, LANES)], store_sem.at[f, q])

    def step(q):
        chunk(odd, even, last, MARGIN + q * LANES, [WIDE] * (LANES // WIDE), False, False)

    def write(q):
        words = pl.ds(MARGIN + q * LANES, LANES)
        for s in range(PLANES):
            lines = pl.ds(s, LANES, stride=PLANES)
            u_now = even[s + 1, words, :]
            u_nat[q, lines, :] = jnp.transpose(4.0 * u_now)
            v_nat[q, lines, :] = jnp.transpose(8.0 * (u_now - odd[s + 1, words, :]))
        for f in (0, 1):
            store(f, q).start()

    step(0)
    for q in range(1, blocks):
        step(q)
        write(q - 1)
    write(blocks - 1)
    for q in range(blocks):
        for f in (0, 1):
            store(f, q).wait()


def solution(mesh):
    n_row, n_col = mesh.shape["row"], mesh.shape["col"]
    tile_spec = P(("ens", "row"), "col")

    def local_run(u_tile, v_tile, stencil_w):
        rows, cols = u_tile.shape
        steps = stencil_w.shape[0]
        blocks = cols // LANES
        assert rows + 2 * HALO == LANES * PLANES and steps % 2 == 0 and steps < HALO
        native = pltpu.VMEM((blocks, rows + 2 * HALO, LANES), jnp.float32)
        level = jax.ShapeDtypeStruct((PLANES + 2, cols + 2 * MARGIN, LANES), jnp.float32)
        hbm, vmem = pl.BlockSpec(memory_space=pltpu.HBM), pl.BlockSpec(memory_space=pltpu.VMEM)
        tile = jax.ShapeDtypeStruct((rows, cols), jnp.float32)
        dma = pltpu.SemaphoreType.DMA
        pairs = min(6, steps // 4, (cols - 2 * INNER - 128) // (4 * STAGE))
        w_rows = jax.ShapeDtypeStruct((steps, 8, LANES), jnp.float32)
        state = pl.pallas_call(
            functools.partial(start, n_row, n_col, steps, pairs),
            out_shape=(level, level, w_rows),
            in_specs=[hbm, hbm, hbm],
            out_specs=(vmem, vmem, vmem),
            scratch_shapes=[
                native, native, pltpu.SMEM((3, 3, steps), jnp.float32), dma((2, blocks)), dma(()),
                dma((2, 2, blocks)), dma((2, 2, blocks)), dma((2, 2)), dma((2, 2)),
            ],
            compiler_params=pltpu.CompilerParams(
                collective_id=0, has_side_effects=True, vmem_limit_bytes=26 * 2**20),
            name="start",
        )(*(pltpu.with_memory_space_constraint(x, pltpu.HBM) for x in (u_tile, v_tile, jnp.transpose(stencil_w, (1, 2, 0)))))
        return pl.pallas_call(
            functools.partial(finish, steps, 2 * pairs),
            out_shape=(tile, tile, level, level),
            in_specs=[vmem, vmem, vmem],
            out_specs=(hbm, hbm, vmem, vmem),
            input_output_aliases={0: 2, 1: 3},
            scratch_shapes=[native, native, dma((2, blocks))],
            compiler_params=pltpu.CompilerParams(vmem_limit_bytes=26 * 2**20),
            name="finish",
        )(*state)[:2]

    return jax.shard_map(
        local_run, mesh=mesh, in_specs=(tile_spec, tile_spec, P()), out_specs=(tile_spec, tile_spec), check_vma=False)
```

```python
import functools

import jax
import jax.numpy as jnp
from jax import lax
from jax.experimental import pallas as pl
from jax.experimental.pallas import tpu as pltpu
from jax.sharding import PartitionSpec as P

LANES = 128
PLANES = 9
HALO = 64
MARGIN = 128
INNER = 96
STAGE = 16
WIDE = 32
PARTS = 2
BLOCKS = (8, 4, 1)
TAPS = 5


def step_weights(w_ref, t):
    return (
        1.5 + 0.5 * w_ref[1, 1, t],
        0.5 * w_ref[0, 0, t],
        0.5 * w_ref[0, 1, t],
        0.5 * w_ref[0, 2, t],
        0.5 * w_ref[1, 0, t],
    )


def chunk(now, old, weights, start, widths, left_ghosts, own_ghosts):
    centre, w00, w01, w02, w10 = weights
    blocks = [(sum(widths[:i]), width) for i, width in enumerate(widths)]

    def taps(block, p):
        return [now[p, pl.ds(start + (block[0] + d), block[1]), :] for d in (-1, 0, 1)]

    def update(block, p, up, mid, down):
        cols = pl.ds(start + block[0], block[1])
        new = (
            (centre * mid[1] - old[p, cols, :])
            + w01 * (up[1] + down[1])
            + w10 * (mid[0] + mid[2])
            + w00 * (up[0] + down[2])
            + w02 * (up[2] + down[0])
        )
        old[p, cols, :] = new
        return new

    ghosts = []
    if left_ghosts:
        cols = pl.ds(start - WIDE, WIDE)
        ghosts.append((cols, pltpu.roll(old[PLANES, cols, :], 1, 1), pltpu.roll(old[1, cols, :], LANES - 1, 1)))
    for b in blocks:
        cols = pl.ds(start + b[0], b[1])
        last = update(b, PLANES, taps(b, PLANES - 1), taps(b, PLANES), taps(b, PLANES + 1))
        first = update(b, 1, taps(b, 0), taps(b, 1), taps(b, 2))
        if own_ghosts:
            ghosts.append((cols, pltpu.roll(last, 1, 1), pltpu.roll(first, LANES - 1, 1)))
    for b in blocks:
        up, mid = taps(b, 1), taps(b, 2)
        for p in range(2, PLANES):
            down = taps(b, p + 1)
            update(b, p, up, mid, down)
            up, mid = mid, down
    for cols, top, bottom in ghosts:
        old[0, cols, :] = top
        old[PLANES + 1, cols, :] = bottom


def sweep(now, old, weights, first_col, width):
    done = first_col + MARGIN
    left = width
    counts = []
    for blocks in BLOCKS:
        counts.append((blocks, lax.div(left, WIDE * blocks)))
        left = left - counts[-1][1] * (WIDE * blocks)
    for blocks, count in reversed(counts):
        size = WIDE * blocks

        def body(i, carry, done=done, blocks=blocks, size=size):
            chunk(now, old, weights, pl.multiple_of(done + i * size, 8), [WIDE] * blocks, True, blocks > 1)
            return carry

        lax.fori_loop(0, count, body, 0)
        done = done + count * size


def wide_sweep(now, old, weights, cols, extra):
    part = (cols + 2 * extra) // PARTS
    widths = [WIDE] * (part // WIDE - 1)
    widths.append(part - sum(widths))

    def body(i, carry):
        chunk(now, old, weights, pl.multiple_of(MARGIN - extra + i * part, 8), widths, False, True)
        return carry

    lax.fori_loop(0, PARTS, body, 0)


def start(n_row, n_col, steps, pairs, u_hbm, v_hbm, w_hbm, even, odd, w_rows, u_nat, v_nat, w_ref, load_sem, w_sem,
           row_send, row_recv, col_send, col_recv):
    rows, cols = u_hbm.shape
    blocks = cols // LANES
    row_id, col_id = lax.axis_index("row"), lax.axis_index("col")
    above, below = lax.rem(row_id + n_row - 1, n_row), lax.rem(row_id + 1, n_row)
    left, right = lax.rem(col_id + n_col - 1, n_col), lax.rem(col_id + 1, n_col)

    def load(f, q):
        src, dst = ((u_hbm, u_nat), (v_hbm, v_nat))[f]
        return pltpu.make_async_copy(
            src.at[:, pl.ds(q * LANES, LANES)], dst.at[q, pl.ds(HALO, rows), :], load_sem.at[f, q])

    def row_copy(f, side, q):
        ref = (u_nat, v_nat)[f]
        depth = steps
        lines = (HALO + rows - depth, HALO)[side]
        place = (HALO - depth, HALO + rows)[side]
        return pltpu.make_async_remote_copy(
            src_ref=ref.at[q, pl.ds(lines, depth), :], dst_ref=ref.at[q, pl.ds(place, depth), :],
            send_sem=row_send.at[f, side, q], recv_sem=row_recv.at[f, side, q],
            device_id={"row": (below, above)[side]}, device_id_type=pl.DeviceIdType.MESH)

    def col_copy(f, side):
        ref, planes = (even, odd)[f], pl.ds(1, PLANES)
        depth = steps
        lines = (MARGIN + cols - depth, MARGIN)[side]
        place = (MARGIN - depth, MARGIN + cols)[side]
        return pltpu.make_async_remote_copy(
            src_ref=ref.at[planes, pl.ds(lines, depth), :], dst_ref=ref.at[planes, pl.ds(place, depth), :],
            send_sem=col_send.at[f, side], recv_sem=col_recv.at[f, side],
            device_id={"col": (right, left)[side]}, device_id_type=pl.DeviceIdType.MESH)

    load_weights = pltpu.make_async_copy(w_hbm, w_ref, w_sem)
    load_weights.start()
    order = [0, blocks - 1] + list(range(1, blocks - 1))
    for q in order:
        for f in (0, 1):
            load(f, q).start()

    barrier = pltpu.get_barrier_semaphore()
    for peer in ({"row": above}, {"row": below}, {"col": left}, {"col": right}):
        pl.semaphore_signal(barrier, inc=1, device_id=peer, device_id_type=pl.DeviceIdType.MESH)
    pl.semaphore_wait(barrier, 4)

    for q in order:
        for f in (0, 1):
            load(f, q).wait()
            for side in (0, 1):
                row_copy(f, side, q).start()

    load_weights.wait()

    def spread(t, carry):
        for k, weight in enumerate(step_weights(w_ref, t)):
            w_rows[t, pl.ds(k, 1), :] = jnp.full((1, LANES), weight, jnp.float32)
        return carry

    lax.fori_loop(0, steps, spread, 0)

    for place, q in enumerate(order):
        if place == 3:
            for f in (0, 1):
                for side in (0, 1):
                    col_copy(f, side).start()
        for f in (0, 1):
            for side in (0, 1):
                row_copy(f, side, q).wait()

        for s in range(PLANES):
            lines = pl.ds(s, LANES, stride=PLANES)
            u_now = 0.25 * u_nat[q, lines, :]
            u_old = u_now - 0.125 * v_nat[q, lines, :]
            words = pl.ds(MARGIN + q * LANES, LANES)
            u_now = jnp.transpose(u_now)
            even[s + 1, words, :] = u_now
            odd[s + 1, words, :] = jnp.transpose(u_old)
            if s == 0:
                even[PLANES + 1, words, :] = pltpu.roll(u_now, LANES - 1, 1)
            if s == PLANES - 1:
                even[0, words, :] = pltpu.roll(u_now, 1, 1)

    def advance(step):
        def pair(v, carry):
            for odd_step, (now, old) in enumerate(((even, odd), (odd, even))):
                t = 2 * v + odd_step
                step(now, old, step_weights(w_ref, t), t)
            return carry

        lax.fori_loop(0, pairs, pair, 0)

    def inner(now, old, weights, t):
        begin = INNER + STAGE * t
        sweep(now, old, weights, begin, cols - 2 * begin)

    advance(inner)
    for f in (0, 1):
        for side in (0, 1):
            col_copy(f, side).wait()


def finish(steps, pairs, even_in, odd_in, w_rows, uo_hbm, vo_hbm, even, odd, u_nat, v_nat, store_sem):
    del even_in, odd_in
    rows, cols = uo_hbm.shape
    blocks = cols // LANES

    def weights_of(t):
        return [w_rows[t, pl.ds(k, 1), :] for k in range(TAPS)]

    def pair(v, carry, extra):
        for odd_step, (now, old) in enumerate(((even, odd), (odd, even))):
            wide_sweep(now, old, weights_of(2 * v + odd_step), cols, extra)
        return carry

    for place in (MARGIN - steps, MARGIN + cols):
        words = pl.ds(place, steps)
        even[0, words, :] = pltpu.roll(even[PLANES, words, :], 1, 1)
        even[PLANES + 1, words, :] = pltpu.roll(even[1, words, :], LANES - 1, 1)

    for t in range(2 * pairs):
        now, old = ((even, odd), (odd, even))[t % 2]
        end = INNER + STAGE * t
        width = STAGE * ((end + steps - 1 - t + STAGE - 1) // STAGE)
        widths = [WIDE] * (width // WIDE - 1)
        widths.append(width - sum(widths))

        def side(i, carry, now=now, old=old, t=t, end=end, width=width, widths=widths):
            left = MARGIN + end - width + i * (cols - 2 * end + width)
            chunk(now, old, weights_of(t), pl.multiple_of(left, 8), widths, False, True)
            return carry

        lax.fori_loop(0, 2, side, 0)

    t = 2 * pairs
    while steps - t > 2:
        extra = 8 * ((steps - 1 - t + 7) // 8)
        until = min(steps - 2, steps - 1 - (extra - 8))
        until += until % 2
        until = min(until, steps - 2)
        lax.fori_loop(t // 2, until // 2, functools.partial(pair, extra=extra), 0)
        t = until
    wide_sweep(even, odd, weights_of(steps - 2), cols, 8)

    last = weights_of(steps - 1)

    def store(f, q):
        src, dst = ((u_nat, uo_hbm), (v_nat, vo_hbm))[f]
        return pltpu.make_async_copy(
            src.at[q, pl.ds(HALO, rows), :],
            dst.at[:, pl.ds(q * LANES, LANES)], store_sem.at[f, q])

    def step(q):
        chunk(odd, even, last, MARGIN + q * LANES, [WIDE] * (LANES // WIDE), False, False)

    def write(q):
        words = pl.ds(MARGIN + q * LANES, LANES)
        for s in range(PLANES):
            lines = pl.ds(s, LANES, stride=PLANES)
            u_now = even[s + 1, words, :]
            u_nat[q, lines, :] = jnp.transpose(4.0 * u_now)
            v_nat[q, lines, :] = jnp.transpose(8.0 * (u_now - odd[s + 1, words, :]))
        for f in (0, 1):
            store(f, q).start()

    step(0)
    for q in range(1, blocks):
        step(q)
        write(q - 1)
    write(blocks - 1)
    for q in range(blocks):
        for f in (0, 1):
            store(f, q).wait()


def solution(mesh):
    n_row, n_col = mesh.shape["row"], mesh.shape["col"]
    tile_spec = P(("ens", "row"), "col")

    def local_run(u_tile, v_tile, stencil_w):
        rows, cols = u_tile.shape
        steps = stencil_w.shape[0]
        blocks = cols // LANES
        assert rows + 2 * HALO == LANES * PLANES and steps % 2 == 0 and steps < HALO
        native = pltpu.VMEM((blocks, rows + 2 * HALO, LANES), jnp.float32)
        level = jax.ShapeDtypeStruct((PLANES + 2, cols + 2 * MARGIN, LANES), jnp.float32)
        hbm, vmem = pl.BlockSpec(memory_space=pltpu.HBM), pl.BlockSpec(memory_space=pltpu.VMEM)
        tile = jax.ShapeDtypeStruct((rows, cols), jnp.float32)
        dma = pltpu.SemaphoreType.DMA
        pairs = min(6, steps // 4, (cols - 2 * INNER - 128) // (4 * STAGE))
        w_rows = jax.ShapeDtypeStruct((steps, 8, LANES), jnp.float32)
        state = pl.pallas_call(
            functools.partial(start, n_row, n_col, steps, pairs),
            out_shape=(level, level, w_rows),
            in_specs=[hbm, hbm, hbm],
            out_specs=(vmem, vmem, vmem),
            scratch_shapes=[
                native, native, pltpu.SMEM((3, 3, steps), jnp.float32), dma((2, blocks)), dma(()),
                dma((2, 2, blocks)), dma((2, 2, blocks)), dma((2, 2)), dma((2, 2)),
            ],
            compiler_params=pltpu.CompilerParams(
                collective_id=0, has_side_effects=True, vmem_limit_bytes=26 * 2**20),
            name="start",
        )(*(pltpu.with_memory_space_constraint(x, pltpu.HBM) for x in (u_tile, v_tile, jnp.transpose(stencil_w, (1, 2, 0)))))
        return pl.pallas_call(
            functools.partial(finish, steps, pairs),
            out_shape=(tile, tile, level, level),
            in_specs=[vmem, vmem, vmem],
            out_specs=(hbm, hbm, vmem, vmem),
            input_output_aliases={0: 2, 1: 3},
            scratch_shapes=[native, native, dma((2, blocks))],
            compiler_params=pltpu.CompilerParams(vmem_limit_bytes=26 * 2**20),
            name="finish",
        )(*state)[:2]

    return jax.shard_map(
        local_run, mesh=mesh, in_specs=(tile_spec, tile_spec, P()), out_specs=(tile_spec, tile_spec), check_vma=False)
```

```python
import functools

import jax
import jax.numpy as jnp
from jax import lax
from jax.experimental import pallas as pl
from jax.experimental.pallas import tpu as pltpu
from jax.sharding import PartitionSpec as P

LANES = 128
PLANES = 9
HALO = 64
MARGIN = 128
INNER = 96
STAGE = 16
WIDE = 32
PARTS = 2
BLOCKS = (8, 4, 1)
TAPS = 5


def step_weights(w_ref, t):
    return (
        1.5 + 0.5 * w_ref[1, 1, t],
        0.5 * w_ref[0, 0, t],
        0.5 * w_ref[0, 1, t],
        0.5 * w_ref[0, 2, t],
        0.5 * w_ref[1, 0, t],
    )


def chunk(now, old, weights, start, widths, left_ghosts, own_ghosts):
    centre, w00, w01, w02, w10 = weights
    blocks = [(sum(widths[:i]), width) for i, width in enumerate(widths)]

    def taps(block, p):
        return [now[p, pl.ds(start + (block[0] + d), block[1]), :] for d in (-1, 0, 1)]

    def update(block, p, up, mid, down):
        cols = pl.ds(start + block[0], block[1])
        new = (
            (centre * mid[1] - old[p, cols, :])
            + w01 * (up[1] + down[1])
            + w10 * (mid[0] + mid[2])
            + w00 * (up[0] + down[2])
            + w02 * (up[2] + down[0])
        )
        old[p, cols, :] = new
        return new

    ghosts = []
    if left_ghosts:
        cols = pl.ds(start - WIDE, WIDE)
        ghosts.append((cols, pltpu.roll(old[PLANES, cols, :], 1, 1), pltpu.roll(old[1, cols, :], LANES - 1, 1)))
    for b in blocks:
        cols = pl.ds(start + b[0], b[1])
        last = update(b, PLANES, taps(b, PLANES - 1), taps(b, PLANES), taps(b, PLANES + 1))
        first = update(b, 1, taps(b, 0), taps(b, 1), taps(b, 2))
        if own_ghosts:
            ghosts.append((cols, pltpu.roll(last, 1, 1), pltpu.roll(first, LANES - 1, 1)))
    for b in blocks:
        up, mid = taps(b, 1), taps(b, 2)
        for p in range(2, PLANES):
            down = taps(b, p + 1)
            update(b, p, up, mid, down)
            up, mid = mid, down
    for cols, top, bottom in ghosts:
        old[0, cols, :] = top
        old[PLANES + 1, cols, :] = bottom


def sweep(now, old, weights, first_col, width):
    done = first_col + MARGIN
    left = width
    counts = []
    for blocks in BLOCKS:
        counts.append((blocks, lax.div(left, WIDE * blocks)))
        left = left - counts[-1][1] * (WIDE * blocks)
    for blocks, count in reversed(counts):
        size = WIDE * blocks

        def body(i, carry, done=done, blocks=blocks, size=size):
            chunk(now, old, weights, pl.multiple_of(done + i * size, 8), [WIDE] * blocks, True, blocks > 1)
            return carry

        lax.fori_loop(0, count, body, 0)
        done = done + count * size


def wide_sweep(now, old, weights, cols, extra):
    part = (cols + 2 * extra) // PARTS
    widths = [WIDE] * (part // WIDE - 1)
    widths.append(part - sum(widths))

    def body(i, carry):
        chunk(now, old, weights, pl.multiple_of(MARGIN - extra + i * part, 8), widths, False, True)
        return carry

    lax.fori_loop(0, PARTS, body, 0)


def start(n_row, n_col, steps, pairs, u_hbm, v_hbm, w_hbm, even, odd, w_rows, u_nat, v_nat, w_ref, load_sem, w_sem,
           row_send, row_recv, col_send, col_recv):
    rows, cols = u_hbm.shape
    blocks = cols // LANES
    row_id, col_id = lax.axis_index("row"), lax.axis_index("col")
    above, below = lax.rem(row_id + n_row - 1, n_row), lax.rem(row_id + 1, n_row)
    left, right = lax.rem(col_id + n_col - 1, n_col), lax.rem(col_id + 1, n_col)

    def load(f, q):
        src, dst = ((u_hbm, u_nat), (v_hbm, v_nat))[f]
        return pltpu.make_async_copy(
            src.at[:, pl.ds(q * LANES, LANES)], dst.at[q, pl.ds(HALO, rows), :], load_sem.at[f, q])

    def row_copy(f, side, q):
        ref = (u_nat, v_nat)[f]
        depth = steps
        lines = (HALO + rows - depth, HALO)[side]
        place = (HALO - depth, HALO + rows)[side]
        return pltpu.make_async_remote_copy(
            src_ref=ref.at[q, pl.ds(lines, depth), :], dst_ref=ref.at[q, pl.ds(place, depth), :],
            send_sem=row_send.at[f, side, q], recv_sem=row_recv.at[f, side, q],
            device_id={"row": (below, above)[side]}, device_id_type=pl.DeviceIdType.MESH)

    def col_copy(f, side):
        ref, planes = (even, odd)[f], pl.ds(1, PLANES)
        depth = steps
        lines = (MARGIN + cols - depth, MARGIN)[side]
        place = (MARGIN - depth, MARGIN + cols)[side]
        return pltpu.make_async_remote_copy(
            src_ref=ref.at[planes, pl.ds(lines, depth), :], dst_ref=ref.at[planes, pl.ds(place, depth), :],
            send_sem=col_send.at[f, side], recv_sem=col_recv.at[f, side],
            device_id={"col": (right, left)[side]}, device_id_type=pl.DeviceIdType.MESH)

    load_weights = pltpu.make_async_copy(w_hbm, w_ref, w_sem)
    load_weights.start()
    order = [0, blocks - 1] + list(range(1, blocks - 1))
    for q in order:
        for f in (0, 1):
            load(f, q).start()

    barrier = pltpu.get_barrier_semaphore()
    for peer in ({"row": above}, {"row": below}, {"col": left}, {"col": right}):
        pl.semaphore_signal(barrier, inc=1, device_id=peer, device_id_type=pl.DeviceIdType.MESH)
    pl.semaphore_wait(barrier, 4)

    for q in order:
        for f in (0, 1):
            load(f, q).wait()
            for side in (0, 1):
                row_copy(f, side, q).start()

    load_weights.wait()

    def spread(t, carry):
        for k, weight in enumerate(step_weights(w_ref, t)):
            w_rows[t, pl.ds(k, 1), :] = jnp.full((1, LANES), weight, jnp.float32)
        return carry

    lax.fori_loop(0, steps, spread, 0)

    def take_rows(q):
        for f in (0, 1):
            for side in (0, 1):
                row_copy(f, side, q).wait()

    def lay_out(q):
        words = pl.ds(pl.multiple_of(MARGIN + q * LANES, LANES), LANES)
        for s in range(PLANES):
            lines = pl.ds(s, LANES, stride=PLANES)
            u_now = 0.25 * u_nat[q, lines, :]
            u_old = u_now - 0.125 * v_nat[q, lines, :]
            u_now = jnp.transpose(u_now)
            even[s + 1, words, :] = u_now
            odd[s + 1, words, :] = jnp.transpose(u_old)
            if s == 0:
                even[PLANES + 1, words, :] = pltpu.roll(u_now, LANES - 1, 1)
            if s == PLANES - 1:
                even[0, words, :] = pltpu.roll(u_now, 1, 1)

    def first_step(q, widths):
        begin = pl.multiple_of(MARGIN + INNER + (q - 1) * LANES, 8)
        chunk(even, odd, step_weights(w_ref, 0), begin, widths, False, True)

    take_rows(0)
    lay_out(0)
    take_rows(blocks - 1)
    for f in (0, 1):
        col_copy(f, 1).start()
    lay_out(blocks - 1)
    take_rows(1)
    for f in (0, 1):
        col_copy(f, 0).start()
    lay_out(1)
    first_step(1, [WIDE] * (LANES // WIDE))

    def next_block(q, carry):
        take_rows(q)
        lay_out(q)
        first_step(q, [WIDE] * (LANES // WIDE))
        return carry

    lax.fori_loop(2, blocks - 1, next_block, 0)
    first_step(blocks - 1, [WIDE] * ((2 * LANES - 2 * INNER) // WIDE))

    def advance(step):
        def pair(v, carry):
            for odd_step, (now, old) in enumerate(((even, odd), (odd, even))):
                t = 2 * v + odd_step
                step(now, old, step_weights(w_ref, t), t)
            return carry

        lax.fori_loop(0, pairs, pair, 0)

    def inner(now, old, weights, t):
        begin = INNER + STAGE * t
        sweep(now, old, weights, begin, jnp.where(t == 0, 0, cols - 2 * begin))

    advance(inner)
    for f in (0, 1):
        for side in (0, 1):
            col_copy(f, side).wait()


def finish(steps, pairs, even_in, odd_in, w_rows, uo_hbm, vo_hbm, even, odd, u_nat, v_nat, store_sem):
    del even_in, odd_in
    rows, cols = uo_hbm.shape
    blocks = cols // LANES

    def weights_of(t):
        return [w_rows[t, pl.ds(k, 1), :] for k in range(TAPS)]

    def pair(v, carry, extra):
        for odd_step, (now, old) in enumerate(((even, odd), (odd, even))):
            wide_sweep(now, old, weights_of(2 * v + odd_step), cols, extra)
        return carry

    for place in (MARGIN - steps, MARGIN + cols):
        words = pl.ds(place, steps)
        even[0, words, :] = pltpu.roll(even[PLANES, words, :], 1, 1)
        even[PLANES + 1, words, :] = pltpu.roll(even[1, words, :], LANES - 1, 1)

    for t in range(2 * pairs):
        now, old = ((even, odd), (odd, even))[t % 2]
        end = INNER + STAGE * t
        width = STAGE * ((end + steps - 1 - t + STAGE - 1) // STAGE)
        widths = [WIDE] * (width // WIDE - 1)
        widths.append(width - sum(widths))

        def side(i, carry, now=now, old=old, t=t, end=end, width=width, widths=widths):
            left = MARGIN + end - width + i * (cols - 2 * end + width)
            chunk(now, old, weights_of(t), pl.multiple_of(left, 8), widths, False, True)
            return carry

        lax.fori_loop(0, 2, side, 0)

    t = 2 * pairs
    while steps - t > 2:
        extra = 8 * ((steps - 1 - t + 7) // 8)
        until = min(steps - 2, steps - 1 - (extra - 8))
        until += until % 2
        until = min(until, steps - 2)
        lax.fori_loop(t // 2, until // 2, functools.partial(pair, extra=extra), 0)
        t = until
    wide_sweep(even, odd, weights_of(steps - 2), cols, 8)

    last = weights_of(steps - 1)

    def store(f, q):
        src, dst = ((u_nat, uo_hbm), (v_nat, vo_hbm))[f]
        return pltpu.make_async_copy(
            src.at[q, pl.ds(HALO, rows), :],
            dst.at[:, pl.ds(q * LANES, LANES)], store_sem.at[f, q])

    def step(q):
        chunk(odd, even, last, MARGIN + q * LANES, [WIDE] * (LANES // WIDE), False, False)

    def write(q):
        words = pl.ds(MARGIN + q * LANES, LANES)
        for s in range(PLANES):
            lines = pl.ds(s, LANES, stride=PLANES)
            u_now = even[s + 1, words, :]
            u_nat[q, lines, :] = jnp.transpose(4.0 * u_now)
            v_nat[q, lines, :] = jnp.transpose(8.0 * (u_now - odd[s + 1, words, :]))
        for f in (0, 1):
            store(f, q).start()

    step(0)
    for q in range(1, blocks):
        step(q)
        write(q - 1)
    write(blocks - 1)
    for q in range(blocks):
        for f in (0, 1):
            store(f, q).wait()


def solution(mesh):
    n_row, n_col = mesh.shape["row"], mesh.shape["col"]
    tile_spec = P(("ens", "row"), "col")

    def local_run(u_tile, v_tile, stencil_w):
        rows, cols = u_tile.shape
        steps = stencil_w.shape[0]
        blocks = cols // LANES
        assert rows + 2 * HALO == LANES * PLANES and steps % 2 == 0 and steps < HALO
        native = pltpu.VMEM((blocks, rows + 2 * HALO, LANES), jnp.float32)
        level = jax.ShapeDtypeStruct((PLANES + 2, cols + 2 * MARGIN, LANES), jnp.float32)
        hbm, vmem = pl.BlockSpec(memory_space=pltpu.HBM), pl.BlockSpec(memory_space=pltpu.VMEM)
        tile = jax.ShapeDtypeStruct((rows, cols), jnp.float32)
        dma = pltpu.SemaphoreType.DMA
        pairs = min(7, steps // 4, (cols - 2 * INNER - 128) // (4 * STAGE))
        w_rows = jax.ShapeDtypeStruct((steps, 8, LANES), jnp.float32)
        state = pl.pallas_call(
            functools.partial(start, n_row, n_col, steps, pairs),
            out_shape=(level, level, w_rows),
            in_specs=[hbm, hbm, hbm],
            out_specs=(vmem, vmem, vmem),
            scratch_shapes=[
                native, native, pltpu.SMEM((3, 3, steps), jnp.float32), dma((2, blocks)), dma(()),
                dma((2, 2, blocks)), dma((2, 2, blocks)), dma((2, 2)), dma((2, 2)),
            ],
            compiler_params=pltpu.CompilerParams(
                collective_id=0, has_side_effects=True, vmem_limit_bytes=26 * 2**20),
            name="start",
        )(*(pltpu.with_memory_space_constraint(x, pltpu.HBM) for x in (u_tile, v_tile, jnp.transpose(stencil_w, (1, 2, 0)))))
        return pl.pallas_call(
            functools.partial(finish, steps, pairs),
            out_shape=(tile, tile, level, level),
            in_specs=[vmem, vmem, vmem],
            out_specs=(hbm, hbm, vmem, vmem),
            input_output_aliases={0: 2, 1: 3},
            scratch_shapes=[native, native, dma((2, blocks))],
            compiler_params=pltpu.CompilerParams(vmem_limit_bytes=26 * 2**20),
            name="finish",
        )(*state)[:2]

    return jax.shard_map(
        local_run, mesh=mesh, in_specs=(tile_spec, tile_spec, P()), out_specs=(tile_spec, tile_spec), check_vma=False)
```

```python
import functools

import jax
import jax.numpy as jnp
from jax import lax
from jax.experimental import pallas as pl
from jax.experimental.pallas import tpu as pltpu
from jax.sharding import PartitionSpec as P

LANES = 128
PLANES = 9
HALO = 64
MARGIN = 128
INNER = 96
STAGE = 16
WIDE = 32
PARTS = 2
BLOCKS = (8, 4, 1)
TAPS = 5


def step_weights(w_ref, t):
    return (
        1.5 + 0.5 * w_ref[1, 1, t],
        0.5 * w_ref[0, 0, t],
        0.5 * w_ref[0, 1, t],
        0.5 * w_ref[0, 2, t],
        0.5 * w_ref[1, 0, t],
    )


def chunk(now, old, weights, start, widths, left_ghosts, own_ghosts):
    centre, w00, w01, w02, w10 = weights
    blocks = [(sum(widths[:i]), width) for i, width in enumerate(widths)]

    def taps(block, p):
        return [now[p, pl.ds(start + (block[0] + d), block[1]), :] for d in (-1, 0, 1)]

    def update(block, p, up, mid, down):
        cols = pl.ds(start + block[0], block[1])
        new = (
            (centre * mid[1] - old[p, cols, :])
            + w01 * (up[1] + down[1])
            + w10 * (mid[0] + mid[2])
            + w00 * (up[0] + down[2])
            + w02 * (up[2] + down[0])
        )
        old[p, cols, :] = new
        return new

    ghosts = []
    if left_ghosts:
        cols = pl.ds(start - WIDE, WIDE)
        ghosts.append((cols, pltpu.roll(old[PLANES, cols, :], 1, 1), pltpu.roll(old[1, cols, :], LANES - 1, 1)))
    for b in blocks:
        cols = pl.ds(start + b[0], b[1])
        last = update(b, PLANES, taps(b, PLANES - 1), taps(b, PLANES), taps(b, PLANES + 1))
        first = update(b, 1, taps(b, 0), taps(b, 1), taps(b, 2))
        if own_ghosts:
            ghosts.append((cols, pltpu.roll(last, 1, 1), pltpu.roll(first, LANES - 1, 1)))
    for b in blocks:
        up, mid = taps(b, 1), taps(b, 2)
        for p in range(2, PLANES):
            down = taps(b, p + 1)
            update(b, p, up, mid, down)
            up, mid = mid, down
    for cols, top, bottom in ghosts:
        old[0, cols, :] = top
        old[PLANES + 1, cols, :] = bottom


def sweep(now, old, weights, first_col, width):
    done = first_col + MARGIN
    left = width
    counts = []
    for blocks in BLOCKS:
        counts.append((blocks, lax.div(left, WIDE * blocks)))
        left = left - counts[-1][1] * (WIDE * blocks)
    for blocks, count in reversed(counts):
        size = WIDE * blocks

        def body(i, carry, done=done, blocks=blocks, size=size):
            chunk(now, old, weights, pl.multiple_of(done + i * size, 8), [WIDE] * blocks, True, blocks > 1)
            return carry

        lax.fori_loop(0, count, body, 0)
        done = done + count * size


def wide_sweep(now, old, weights, cols, extra):
    part = (cols + 2 * extra) // PARTS
    widths = [WIDE] * (part // WIDE - 1)
    widths.append(part - sum(widths))

    def body(i, carry):
        chunk(now, old, weights, pl.multiple_of(MARGIN - extra + i * part, 8), widths, False, True)
        return carry

    lax.fori_loop(0, PARTS, body, 0)


def start(n_row, n_col, steps, pairs, u_hbm, v_hbm, w_hbm, even, odd, w_rows, u_nat, v_nat, w_ref, load_sem, w_sem,
           row_send, row_recv, col_send, col_recv):
    rows, cols = u_hbm.shape
    blocks = cols // LANES
    row_id, col_id = lax.axis_index("row"), lax.axis_index("col")
    above, below = lax.rem(row_id + n_row - 1, n_row), lax.rem(row_id + 1, n_row)
    left, right = lax.rem(col_id + n_col - 1, n_col), lax.rem(col_id + 1, n_col)

    def load(f, q):
        src, dst = ((u_hbm, u_nat), (v_hbm, v_nat))[f]
        return pltpu.make_async_copy(
            src.at[:, pl.ds(q * LANES, LANES)], dst.at[q, pl.ds(HALO, rows), :], load_sem.at[f, q])

    def row_copy(f, side, q):
        ref = (u_nat, v_nat)[f]
        depth = steps
        lines = (HALO + rows - depth, HALO)[side]
        place = (HALO - depth, HALO + rows)[side]
        return pltpu.make_async_remote_copy(
            src_ref=ref.at[q, pl.ds(lines, depth), :], dst_ref=ref.at[q, pl.ds(place, depth), :],
            send_sem=row_send.at[f, side, q], recv_sem=row_recv.at[f, side, q],
            device_id={"row": (below, above)[side]}, device_id_type=pl.DeviceIdType.MESH)

    def col_copy(f, side):
        ref, planes = (even, odd)[f], pl.ds(1, PLANES)
        depth = steps
        lines = (MARGIN + cols - depth, MARGIN)[side]
        place = (MARGIN - depth, MARGIN + cols)[side]
        return pltpu.make_async_remote_copy(
            src_ref=ref.at[planes, pl.ds(lines, depth), :], dst_ref=ref.at[planes, pl.ds(place, depth), :],
            send_sem=col_send.at[f, side], recv_sem=col_recv.at[f, side],
            device_id={"col": (right, left)[side]}, device_id_type=pl.DeviceIdType.MESH)

    load_weights = pltpu.make_async_copy(w_hbm, w_ref, w_sem)
    load_weights.start()
    order = [0, blocks - 1] + list(range(1, blocks - 1))
    for q in order:
        for f in (0, 1):
            load(f, q).start()

    barrier = pltpu.get_barrier_semaphore()
    for peer in ({"row": above}, {"row": below}, {"col": left}, {"col": right}):
        pl.semaphore_signal(barrier, inc=1, device_id=peer, device_id_type=pl.DeviceIdType.MESH)
    pl.semaphore_wait(barrier, 4)

    for q in order:
        for f in (0, 1):
            load(f, q).wait()
            for side in (0, 1):
                row_copy(f, side, q).start()

    load_weights.wait()

    def spread(t, carry):
        for k, weight in enumerate(step_weights(w_ref, t)):
            w_rows[t, pl.ds(k, 1), :] = jnp.full((1, LANES), weight, jnp.float32)
        return carry

    lax.fori_loop(0, steps, spread, 0)

    def take_rows(q):
        for f in (0, 1):
            for side in (0, 1):
                row_copy(f, side, q).wait()

    def lay_out(q):
        words = pl.ds(pl.multiple_of(MARGIN + q * LANES, LANES), LANES)
        for s in range(PLANES):
            lines = pl.ds(s, LANES, stride=PLANES)
            u_now = 0.25 * u_nat[q, lines, :]
            u_old = u_now - 0.125 * v_nat[q, lines, :]
            u_now = jnp.transpose(u_now)
            even[s + 1, words, :] = u_now
            odd[s + 1, words, :] = jnp.transpose(u_old)
            if s == 0:
                even[PLANES + 1, words, :] = pltpu.roll(u_now, LANES - 1, 1)
            if s == PLANES - 1:
                even[0, words, :] = pltpu.roll(u_now, 1, 1)

    def first_step(q, widths):
        begin = pl.multiple_of(MARGIN + INNER + (q - 1) * LANES, 8)
        chunk(even, odd, step_weights(w_ref, 0), begin, widths, False, True)

    take_rows(0)
    lay_out(0)
    take_rows(blocks - 1)
    for f in (0, 1):
        col_copy(f, 1).start()
    lay_out(blocks - 1)
    take_rows(1)
    for f in (0, 1):
        col_copy(f, 0).start()
    lay_out(1)

    def ready_step(q, carry):
        first_step(q, [WIDE] * (LANES // WIDE))
        return carry

    def next_block(q, carry):
        lax.fori_loop(q - 1, q, ready_step, 0)
        take_rows(q)
        lay_out(q)
        return carry

    lax.fori_loop(2, blocks - 1, next_block, 0)
    first_step(blocks - 2, [WIDE] * (LANES // WIDE))
    first_step(blocks - 1, [WIDE] * ((2 * LANES - 2 * INNER) // WIDE))

    def advance(step):
        def pair(v, carry):
            for odd_step, (now, old) in enumerate(((even, odd), (odd, even))):
                t = 2 * v + odd_step
                step(now, old, step_weights(w_ref, t), t)
            return carry

        lax.fori_loop(0, pairs, pair, 0)

    def inner(now, old, weights, t):
        begin = INNER + STAGE * t
        sweep(now, old, weights, begin, jnp.where(t == 0, 0, cols - 2 * begin))

    advance(inner)
    for f in (0, 1):
        for side in (0, 1):
            col_copy(f, side).wait()


def finish(steps, pairs, even_in, odd_in, w_rows, uo_hbm, vo_hbm, even, odd, u_nat, v_nat, store_sem):
    del even_in, odd_in
    rows, cols = uo_hbm.shape
    blocks = cols // LANES

    def weights_of(t):
        return [w_rows[t, pl.ds(k, 1), :] for k in range(TAPS)]

    def pair(v, carry, extra):
        for odd_step, (now, old) in enumerate(((even, odd), (odd, even))):
            wide_sweep(now, old, weights_of(2 * v + odd_step), cols, extra)
        return carry

    for place in (MARGIN - steps, MARGIN + cols):
        words = pl.ds(place, steps)
        even[0, words, :] = pltpu.roll(even[PLANES, words, :], 1, 1)
        even[PLANES + 1, words, :] = pltpu.roll(even[1, words, :], LANES - 1, 1)

    for t in range(2 * pairs):
        now, old = ((even, odd), (odd, even))[t % 2]
        end = INNER + STAGE * t
        width = STAGE * ((end + steps - 1 - t + STAGE - 1) // STAGE)
        widths = [WIDE] * (width // WIDE - 1)
        widths.append(width - sum(widths))

        def side(i, carry, now=now, old=old, t=t, end=end, width=width, widths=widths):
            left = MARGIN + end - width + i * (cols - 2 * end + width)
            chunk(now, old, weights_of(t), pl.multiple_of(left, 8), widths, False, True)
            return carry

        lax.fori_loop(0, 2, side, 0)

    t = 2 * pairs
    while steps - t > 2:
        extra = 8 * ((steps - 1 - t + 7) // 8)
        until = min(steps - 2, steps - 1 - (extra - 8))
        until += until % 2
        until = min(until, steps - 2)
        lax.fori_loop(t // 2, until // 2, functools.partial(pair, extra=extra), 0)
        t = until
    wide_sweep(even, odd, weights_of(steps - 2), cols, 8)

    last = weights_of(steps - 1)

    def store(f, q):
        src, dst = ((u_nat, uo_hbm), (v_nat, vo_hbm))[f]
        return pltpu.make_async_copy(
            src.at[q, pl.ds(HALO, rows), :],
            dst.at[:, pl.ds(q * LANES, LANES)], store_sem.at[f, q])

    def step(q):
        chunk(odd, even, last, MARGIN + q * LANES, [WIDE] * (LANES // WIDE), False, False)

    def write(q):
        words = pl.ds(MARGIN + q * LANES, LANES)
        for s in range(PLANES):
            lines = pl.ds(s, LANES, stride=PLANES)
            u_now = even[s + 1, words, :]
            u_nat[q, lines, :] = jnp.transpose(4.0 * u_now)
            v_nat[q, lines, :] = jnp.transpose(8.0 * (u_now - odd[s + 1, words, :]))
        for f in (0, 1):
            store(f, q).start()

    step(0)
    for q in range(1, blocks):
        step(q)
        write(q - 1)
    write(blocks - 1)
    for q in range(blocks):
        for f in (0, 1):
            store(f, q).wait()


def solution(mesh):
    n_row, n_col = mesh.shape["row"], mesh.shape["col"]
    tile_spec = P(("ens", "row"), "col")

    def local_run(u_tile, v_tile, stencil_w):
        rows, cols = u_tile.shape
        steps = stencil_w.shape[0]
        blocks = cols // LANES
        assert rows + 2 * HALO == LANES * PLANES and steps % 2 == 0 and steps < HALO
        native = pltpu.VMEM((blocks, rows + 2 * HALO, LANES), jnp.float32)
        level = jax.ShapeDtypeStruct((PLANES + 2, cols + 2 * MARGIN, LANES), jnp.float32)
        hbm, vmem = pl.BlockSpec(memory_space=pltpu.HBM), pl.BlockSpec(memory_space=pltpu.VMEM)
        tile = jax.ShapeDtypeStruct((rows, cols), jnp.float32)
        dma = pltpu.SemaphoreType.DMA
        pairs = min(7, steps // 4, (cols - 2 * INNER - 128) // (4 * STAGE))
        w_rows = jax.ShapeDtypeStruct((steps, 8, LANES), jnp.float32)
        state = pl.pallas_call(
            functools.partial(start, n_row, n_col, steps, pairs),
            out_shape=(level, level, w_rows),
            in_specs=[hbm, hbm, hbm],
            out_specs=(vmem, vmem, vmem),
            scratch_shapes=[
                native, native, pltpu.SMEM((3, 3, steps), jnp.float32), dma((2, blocks)), dma(()),
                dma((2, 2, blocks)), dma((2, 2, blocks)), dma((2, 2)), dma((2, 2)),
            ],
            compiler_params=pltpu.CompilerParams(
                collective_id=0, has_side_effects=True, vmem_limit_bytes=26 * 2**20),
            name="start",
        )(*(pltpu.with_memory_space_constraint(x, pltpu.HBM) for x in (u_tile, v_tile, jnp.transpose(stencil_w, (1, 2, 0)))))
        return pl.pallas_call(
            functools.partial(finish, steps, pairs),
            out_shape=(tile, tile, level, level),
            in_specs=[vmem, vmem, vmem],
            out_specs=(hbm, hbm, vmem, vmem),
            input_output_aliases={0: 2, 1: 3},
            scratch_shapes=[native, native, dma((2, blocks))],
            compiler_params=pltpu.CompilerParams(vmem_limit_bytes=26 * 2**20),
            name="finish",
        )(*state)[:2]

    return jax.shard_map(
        local_run, mesh=mesh, in_specs=(tile_spec, tile_spec, P()), out_specs=(tile_spec, tile_spec), check_vma=False)
```

```python
import functools

import jax
import jax.numpy as jnp
from jax import lax
from jax.experimental import pallas as pl
from jax.experimental.pallas import tpu as pltpu
from jax.sharding import PartitionSpec as P

LANES = 128
PLANES = 9
HALO = 64
MARGIN = 128
INNER = 96
STAGE = 16
WIDE = 32
PARTS = 2
BLOCKS = (8, 4, 1)
TAPS = 5


def step_weights(w_ref, t):
    return (
        1.5 + 0.5 * w_ref[1, 1, t],
        0.5 * w_ref[0, 0, t],
        0.5 * w_ref[0, 1, t],
        0.5 * w_ref[0, 2, t],
        0.5 * w_ref[1, 0, t],
    )


def chunk(now, old, weights, start, widths, left_ghosts, own_ghosts):
    centre, w00, w01, w02, w10 = weights
    blocks = [(sum(widths[:i]), width) for i, width in enumerate(widths)]

    def taps(block, p):
        return [now[p, pl.ds(start + (block[0] + d), block[1]), :] for d in (-1, 0, 1)]

    def update(block, p, up, mid, down):
        cols = pl.ds(start + block[0], block[1])
        new = (
            (centre * mid[1] - old[p, cols, :])
            + w01 * (up[1] + down[1])
            + w10 * (mid[0] + mid[2])
            + w00 * (up[0] + down[2])
            + w02 * (up[2] + down[0])
        )
        old[p, cols, :] = new
        return new

    ghosts = []
    if left_ghosts:
        cols = pl.ds(start - WIDE, WIDE)
        ghosts.append((cols, pltpu.roll(old[PLANES, cols, :], 1, 1), pltpu.roll(old[1, cols, :], LANES - 1, 1)))
    for b in blocks:
        cols = pl.ds(start + b[0], b[1])
        last = update(b, PLANES, taps(b, PLANES - 1), taps(b, PLANES), taps(b, PLANES + 1))
        first = update(b, 1, taps(b, 0), taps(b, 1), taps(b, 2))
        if own_ghosts:
            ghosts.append((cols, pltpu.roll(last, 1, 1), pltpu.roll(first, LANES - 1, 1)))
    for b in blocks:
        up, mid = taps(b, 1), taps(b, 2)
        for p in range(2, PLANES):
            down = taps(b, p + 1)
            update(b, p, up, mid, down)
            up, mid = mid, down
    for cols, top, bottom in ghosts:
        old[0, cols, :] = top
        old[PLANES + 1, cols, :] = bottom


def sweep(now, old, weights, first_col, width):
    done = first_col + MARGIN
    left = width
    counts = []
    for blocks in BLOCKS:
        counts.append((blocks, lax.div(left, WIDE * blocks)))
        left = left - counts[-1][1] * (WIDE * blocks)
    for blocks, count in reversed(counts):
        size = WIDE * blocks

        def body(i, carry, done=done, blocks=blocks, size=size):
            chunk(now, old, weights, pl.multiple_of(done + i * size, 8), [WIDE] * blocks, True, blocks > 1)
            return carry

        lax.fori_loop(0, count, body, 0)
        done = done + count * size


def wide_sweep(now, old, weights, cols, extra):
    part = (cols + 2 * extra) // PARTS
    widths = [WIDE] * (part // WIDE - 1)
    widths.append(part - sum(widths))

    def body(i, carry):
        chunk(now, old, weights, pl.multiple_of(MARGIN - extra + i * part, 8), widths, False, True)
        return carry

    lax.fori_loop(0, PARTS, body, 0)


def start(n_row, n_col, steps, pairs, u_hbm, v_hbm, w_hbm, even, odd, w_rows, u_nat, v_nat, w_ref, load_sem, w_sem,
           row_send, row_recv, col_send, col_recv):
    rows, cols = u_hbm.shape
    blocks = cols // LANES
    row_id, col_id = lax.axis_index("row"), lax.axis_index("col")
    above, below = lax.rem(row_id + n_row - 1, n_row), lax.rem(row_id + 1, n_row)
    left, right = lax.rem(col_id + n_col - 1, n_col), lax.rem(col_id + 1, n_col)

    def load(f, q):
        src, dst = ((u_hbm, u_nat), (v_hbm, v_nat))[f]
        return pltpu.make_async_copy(
            src.at[:, pl.ds(q * LANES, LANES)], dst.at[q, pl.ds(HALO, rows), :], load_sem.at[f, q])

    def row_copy(f, side, q):
        ref = (u_nat, v_nat)[f]
        depth = steps
        lines = (HALO + rows - depth, HALO)[side]
        place = (HALO - depth, HALO + rows)[side]
        return pltpu.make_async_remote_copy(
            src_ref=ref.at[q, pl.ds(lines, depth), :], dst_ref=ref.at[q, pl.ds(place, depth), :],
            send_sem=row_send.at[f, side, q], recv_sem=row_recv.at[f, side, q],
            device_id={"row": (below, above)[side]}, device_id_type=pl.DeviceIdType.MESH)

    def col_copy(f, side):
        ref, planes = (even, odd)[f], pl.ds(1, PLANES)
        depth = steps
        lines = (MARGIN + cols - depth, MARGIN)[side]
        place = (MARGIN - depth, MARGIN + cols)[side]
        return pltpu.make_async_remote_copy(
            src_ref=ref.at[planes, pl.ds(lines, depth), :], dst_ref=ref.at[planes, pl.ds(place, depth), :],
            send_sem=col_send.at[f, side], recv_sem=col_recv.at[f, side],
            device_id={"col": (right, left)[side]}, device_id_type=pl.DeviceIdType.MESH)

    load_weights = pltpu.make_async_copy(w_hbm, w_ref, w_sem)
    load_weights.start()
    order = [0, blocks - 1] + list(range(1, blocks - 1))
    for q in order:
        for f in (0, 1):
            load(f, q).start()

    barrier = pltpu.get_barrier_semaphore()
    for peer in ({"row": above}, {"row": below}, {"col": left}, {"col": right}):
        pl.semaphore_signal(barrier, inc=1, device_id=peer, device_id_type=pl.DeviceIdType.MESH)
    pl.semaphore_wait(barrier, 4)

    for q in order:
        for f in (0, 1):
            load(f, q).wait()
            for side in (0, 1):
                row_copy(f, side, q).start()

    load_weights.wait()

    def spread(t, carry):
        for k, weight in enumerate(step_weights(w_ref, t)):
            w_rows[t, pl.ds(k, 1), :] = jnp.full((1, LANES), weight, jnp.float32)
        return carry

    lax.fori_loop(0, steps, spread, 0)

    def take_rows(q):
        for f in (0, 1):
            for side in (0, 1):
                row_copy(f, side, q).wait()

    def lay_out(q):
        words = pl.ds(pl.multiple_of(MARGIN + q * LANES, LANES), LANES)
        for s in range(PLANES):
            lines = pl.ds(s, LANES, stride=PLANES)
            u_now = 0.25 * u_nat[q, lines, :]
            u_old = u_now - 0.125 * v_nat[q, lines, :]
            u_now = jnp.transpose(u_now)
            even[s + 1, words, :] = u_now
            odd[s + 1, words, :] = jnp.transpose(u_old)
            if s == 0:
                even[PLANES + 1, words, :] = pltpu.roll(u_now, LANES - 1, 1)
            if s == PLANES - 1:
                even[0, words, :] = pltpu.roll(u_now, 1, 1)

    def first_step(q, widths):
        begin = pl.multiple_of(MARGIN + INNER + (q - 1) * LANES, 8)
        chunk(even, odd, step_weights(w_ref, 0), begin, widths, False, True)

    take_rows(0)
    lay_out(0)
    take_rows(blocks - 1)
    for f in (0, 1):
        col_copy(f, 1).start()
    lay_out(blocks - 1)
    take_rows(1)
    for f in (0, 1):
        col_copy(f, 0).start()
    lay_out(1)

    def ready_step(q, carry):
        first_step(q, [WIDE] * (LANES // WIDE))
        return carry

    def next_block(q, carry):
        lax.fori_loop(q - 1, q, ready_step, 0)
        take_rows(q)
        lay_out(q)
        return carry

    lax.fori_loop(2, blocks - 1, next_block, 0)
    first_step(blocks - 2, [WIDE] * (LANES // WIDE))
    first_step(blocks - 1, [WIDE] * ((2 * LANES - 2 * INNER) // WIDE))

    def advance(step):
        def pair(v, carry):
            for odd_step, (now, old) in enumerate(((even, odd), (odd, even))):
                t = 2 * v + odd_step
                step(now, old, step_weights(w_ref, t), t)
            return carry

        lax.fori_loop(0, pairs, pair, 0)

    def inner(now, old, weights, t):
        begin = INNER + STAGE * t
        sweep(now, old, weights, begin, jnp.where(t == 0, 0, cols - 2 * begin))

    advance(inner)
    for f in (0, 1):
        for side in (0, 1):
            col_copy(f, side).wait()


def finish(steps, pairs, even_in, odd_in, w_rows, uo_hbm, vo_hbm, even, odd, u_nat, v_nat, store_sem):
    del even_in, odd_in
    rows, cols = uo_hbm.shape
    blocks = cols // LANES

    def weights_of(t):
        return [w_rows[t, pl.ds(k, 1), :] for k in range(TAPS)]

    def pair(v, carry, extra):
        for odd_step, (now, old) in enumerate(((even, odd), (odd, even))):
            wide_sweep(now, old, weights_of(2 * v + odd_step), cols, extra)
        return carry

    for place in (MARGIN - steps, MARGIN + cols):
        words = pl.ds(place, steps)
        even[0, words, :] = pltpu.roll(even[PLANES, words, :], 1, 1)
        even[PLANES + 1, words, :] = pltpu.roll(even[1, words, :], LANES - 1, 1)

    for t in range(2 * pairs):
        now, old = ((even, odd), (odd, even))[t % 2]
        end = INNER + STAGE * t
        width = STAGE * ((end + steps - 1 - t + STAGE - 1) // STAGE)
        widths = [WIDE] * (width // WIDE - 1)
        widths.append(width - sum(widths))

        def side(i, carry, now=now, old=old, t=t, end=end, width=width, widths=widths):
            left = MARGIN + end - width + i * (cols - 2 * end + width)
            chunk(now, old, weights_of(t), pl.multiple_of(left, 8), widths, False, True)
            return carry

        lax.fori_loop(0, 2, side, 0)

    t = 2 * pairs
    while steps - t > 2:
        extra = 8 * ((steps - 1 - t + 7) // 8)
        until = min(steps - 2, steps - 1 - (extra - 8))
        until += until % 2
        until = min(until, steps - 2)
        lax.fori_loop(t // 2, until // 2, functools.partial(pair, extra=extra), 0)
        t = until
    wide_sweep(even, odd, weights_of(steps - 2), cols, 8)

    last = weights_of(steps - 1)

    def store(f, q):
        src, dst = ((u_nat, uo_hbm), (v_nat, vo_hbm))[f]
        return pltpu.make_async_copy(
            src.at[q, pl.ds(HALO, rows), :],
            dst.at[:, pl.ds(q * LANES, LANES)], store_sem.at[f, q])

    def step(q):
        chunk(odd, even, last, MARGIN + q * LANES, [WIDE] * (LANES // WIDE), False, False)

    def write(q):
        words = pl.ds(MARGIN + q * LANES, LANES)
        for s in range(PLANES):
            lines = pl.ds(s, LANES, stride=PLANES)
            u_now = even[s + 1, words, :]
            u_nat[q, lines, :] = jnp.transpose(4.0 * u_now)
            v_nat[q, lines, :] = jnp.transpose(8.0 * (u_now - odd[s + 1, words, :]))
        for f in (0, 1):
            store(f, q).start()

    step(0)
    for q in range(1, blocks):
        step(q)
        write(q - 1)
    write(blocks - 1)
    for q in range(blocks):
        for f in (0, 1):
            store(f, q).wait()


def solution(mesh):
    n_row, n_col = mesh.shape["row"], mesh.shape["col"]
    tile_spec = P(("ens", "row"), "col")

    def local_run(u_tile, v_tile, stencil_w):
        rows, cols = u_tile.shape
        steps = stencil_w.shape[0]
        blocks = cols // LANES
        assert rows + 2 * HALO == LANES * PLANES and steps % 2 == 0 and steps < HALO
        native = pltpu.VMEM((blocks, rows + 2 * HALO, LANES), jnp.float32)
        level = jax.ShapeDtypeStruct((PLANES + 2, cols + 2 * MARGIN, LANES), jnp.float32)
        hbm, vmem = pl.BlockSpec(memory_space=pltpu.HBM), pl.BlockSpec(memory_space=pltpu.VMEM)
        tile = jax.ShapeDtypeStruct((rows, cols), jnp.float32)
        dma = pltpu.SemaphoreType.DMA
        pairs = min(8, steps // 4, (cols - 2 * INNER - 128) // (4 * STAGE))
        w_rows = jax.ShapeDtypeStruct((steps, 8, LANES), jnp.float32)
        state = pl.pallas_call(
            functools.partial(start, n_row, n_col, steps, pairs),
            out_shape=(level, level, w_rows),
            in_specs=[hbm, hbm, hbm],
            out_specs=(vmem, vmem, vmem),
            scratch_shapes=[
                native, native, pltpu.SMEM((3, 3, steps), jnp.float32), dma((2, blocks)), dma(()),
                dma((2, 2, blocks)), dma((2, 2, blocks)), dma((2, 2)), dma((2, 2)),
            ],
            compiler_params=pltpu.CompilerParams(
                collective_id=0, has_side_effects=True, vmem_limit_bytes=26 * 2**20),
            name="start",
        )(*(pltpu.with_memory_space_constraint(x, pltpu.HBM) for x in (u_tile, v_tile, jnp.transpose(stencil_w, (1, 2, 0)))))
        return pl.pallas_call(
            functools.partial(finish, steps, pairs),
            out_shape=(tile, tile, level, level),
            in_specs=[vmem, vmem, vmem],
            out_specs=(hbm, hbm, vmem, vmem),
            input_output_aliases={0: 2, 1: 3},
            scratch_shapes=[native, native, dma((2, blocks))],
            compiler_params=pltpu.CompilerParams(vmem_limit_bytes=26 * 2**20),
            name="finish",
        )(*state)[:2]

    return jax.shard_map(
        local_run, mesh=mesh, in_specs=(tile_spec, tile_spec, P()), out_specs=(tile_spec, tile_spec), check_vma=False)
```

```python
import functools

import jax
import jax.numpy as jnp
from jax import lax
from jax.experimental import pallas as pl
from jax.experimental.pallas import tpu as pltpu
from jax.sharding import PartitionSpec as P

LANES = 128
PLANES = 9
HALO = 64
MARGIN = 128
INNER = 96
STAGE = 16
WIDE = 32
PARTS = 2
BLOCKS = (8, 4, 1)
TAPS = 5


def step_weights(w_ref, t):
    return (
        1.5 + 0.5 * w_ref[1, 1, t],
        0.5 * w_ref[0, 0, t],
        0.5 * w_ref[0, 1, t],
        0.5 * w_ref[0, 2, t],
        0.5 * w_ref[1, 0, t],
    )


def chunk(now, old, weights, start, widths, left_ghosts, own_ghosts):
    centre, w00, w01, w02, w10 = weights
    blocks = [(sum(widths[:i]), width) for i, width in enumerate(widths)]

    def taps(block, p):
        return [now[p, pl.ds(start + (block[0] + d), block[1]), :] for d in (-1, 0, 1)]

    def update(block, p, up, mid, down):
        cols = pl.ds(start + block[0], block[1])
        new = (
            (centre * mid[1] - old[p, cols, :])
            + w01 * (up[1] + down[1])
            + w10 * (mid[0] + mid[2])
            + w00 * (up[0] + down[2])
            + w02 * (up[2] + down[0])
        )
        old[p, cols, :] = new
        return new

    ghosts = []
    if left_ghosts:
        cols = pl.ds(start - WIDE, WIDE)
        ghosts.append((cols, pltpu.roll(old[PLANES, cols, :], 1, 1), pltpu.roll(old[1, cols, :], LANES - 1, 1)))
    for b in blocks:
        cols = pl.ds(start + b[0], b[1])
        last = update(b, PLANES, taps(b, PLANES - 1), taps(b, PLANES), taps(b, PLANES + 1))
        first = update(b, 1, taps(b, 0), taps(b, 1), taps(b, 2))
        if own_ghosts:
            ghosts.append((cols, pltpu.roll(last, 1, 1), pltpu.roll(first, LANES - 1, 1)))
    for b in blocks:
        up, mid = taps(b, 1), taps(b, 2)
        for p in range(2, PLANES):
            down = taps(b, p + 1)
            update(b, p, up, mid, down)
            up, mid = mid, down
    for cols, top, bottom in ghosts:
        old[0, cols, :] = top
        old[PLANES + 1, cols, :] = bottom


def sweep(now, old, weights, first_col, width):
    done = first_col + MARGIN
    left = width
    counts = []
    for blocks in BLOCKS:
        counts.append((blocks, lax.div(left, WIDE * blocks)))
        left = left - counts[-1][1] * (WIDE * blocks)
    for blocks, count in reversed(counts):
        size = WIDE * blocks

        def body(i, carry, done=done, blocks=blocks, size=size):
            chunk(now, old, weights, pl.multiple_of(done + i * size, 8), [WIDE] * blocks, True, blocks > 1)
            return carry

        lax.fori_loop(0, count, body, 0)
        done = done + count * size


def wide_sweep(now, old, weights, cols, extra):
    part = (cols + 2 * extra) // PARTS
    widths = [WIDE] * (part // WIDE - 1)
    widths.append(part - sum(widths))

    def body(i, carry):
        chunk(now, old, weights, pl.multiple_of(MARGIN - extra + i * part, 8), widths, False, True)
        return carry

    lax.fori_loop(0, PARTS, body, 0)


def start(n_row, n_col, steps, pairs, u_hbm, v_hbm, w_hbm, even, odd, w_rows, u_nat, v_nat, w_ref, load_sem, w_sem,
           row_send, row_recv, col_send, col_recv):
    rows, cols = u_hbm.shape
    blocks = cols // LANES
    row_id, col_id = lax.axis_index("row"), lax.axis_index("col")
    above, below = lax.rem(row_id + n_row - 1, n_row), lax.rem(row_id + 1, n_row)
    left, right = lax.rem(col_id + n_col - 1, n_col), lax.rem(col_id + 1, n_col)

    def load(f, q):
        src, dst = ((u_hbm, u_nat), (v_hbm, v_nat))[f]
        return pltpu.make_async_copy(
            src.at[:, pl.ds(q * LANES, LANES)], dst.at[q, pl.ds(HALO, rows), :], load_sem.at[f, q])

    def row_copy(f, side, q):
        ref = (u_nat, v_nat)[f]
        depth = steps
        lines = (HALO + rows - depth, HALO)[side]
        place = (HALO - depth, HALO + rows)[side]
        return pltpu.make_async_remote_copy(
            src_ref=ref.at[q, pl.ds(lines, depth), :], dst_ref=ref.at[q, pl.ds(place, depth), :],
            send_sem=row_send.at[f, side, q], recv_sem=row_recv.at[f, side, q],
            device_id={"row": (below, above)[side]}, device_id_type=pl.DeviceIdType.MESH)

    def col_copy(f, side):
        ref, planes = (even, odd)[f], pl.ds(1, PLANES)
        depth = steps
        lines = (MARGIN + cols - depth, MARGIN)[side]
        place = (MARGIN - depth, MARGIN + cols)[side]
        return pltpu.make_async_remote_copy(
            src_ref=ref.at[planes, pl.ds(lines, depth), :], dst_ref=ref.at[planes, pl.ds(place, depth), :],
            send_sem=col_send.at[f, side], recv_sem=col_recv.at[f, side],
            device_id={"col": (right, left)[side]}, device_id_type=pl.DeviceIdType.MESH)

    load_weights = pltpu.make_async_copy(w_hbm, w_ref, w_sem)
    load_weights.start()
    order = [0, blocks - 1] + list(range(1, blocks - 1))
    for q in order:
        for f in (0, 1):
            load(f, q).start()

    barrier = pltpu.get_barrier_semaphore()
    for peer in ({"row": above}, {"row": below}, {"col": left}, {"col": right}):
        pl.semaphore_signal(barrier, inc=1, device_id=peer, device_id_type=pl.DeviceIdType.MESH)
    pl.semaphore_wait(barrier, 4)

    for q in order:
        for f in (0, 1):
            load(f, q).wait()
            for side in (0, 1):
                row_copy(f, side, q).start()

    load_weights.wait()

    def spread(t, carry):
        for k, weight in enumerate(step_weights(w_ref, t)):
            w_rows[t, pl.ds(k, 1), :] = jnp.full((1, LANES), weight, jnp.float32)
        return carry

    lax.fori_loop(0, steps, spread, 0)

    def take_rows(q):
        for f in (0, 1):
            for side in (0, 1):
                row_copy(f, side, q).wait()

    def lay_out(q):
        words = pl.ds(pl.multiple_of(MARGIN + q * LANES, LANES), LANES)
        for s in range(PLANES):
            lines = pl.ds(s, LANES, stride=PLANES)
            u_now = 0.25 * u_nat[q, lines, :]
            u_old = u_now - 0.125 * v_nat[q, lines, :]
            u_now = jnp.transpose(u_now)
            even[s + 1, words, :] = u_now
            odd[s + 1, words, :] = jnp.transpose(u_old)
            if s == 0:
                even[PLANES + 1, words, :] = pltpu.roll(u_now, LANES - 1, 1)
            if s == PLANES - 1:
                even[0, words, :] = pltpu.roll(u_now, 1, 1)

    def first_step(q, widths):
        begin = pl.multiple_of(MARGIN + INNER + (q - 1) * LANES, 8)
        chunk(even, odd, step_weights(w_ref, 0), begin, widths, False, True)

    def second_step(q, widths):
        begin = pl.multiple_of(MARGIN + INNER + STAGE + (q - 1) * LANES, 8)
        chunk(odd, even, step_weights(w_ref, 1), begin, widths, False, True)

    take_rows(0)
    lay_out(0)
    take_rows(blocks - 1)
    for f in (0, 1):
        col_copy(f, 1).start()
    lay_out(blocks - 1)
    take_rows(1)
    for f in (0, 1):
        col_copy(f, 0).start()
    lay_out(1)

    def ready_step(q, carry):
        first_step(q, [WIDE] * (LANES // WIDE))
        return carry

    def ready_second(q, carry):
        second_step(q, [WIDE] * (LANES // WIDE))
        return carry

    def next_block(q, carry):
        lax.fori_loop(q - 1, q, ready_step, 0)
        lax.fori_loop(jnp.where(q == 2, 1, q - 2), q - 1, ready_second, 0)
        take_rows(q)
        lay_out(q)
        return carry

    lax.fori_loop(2, blocks - 1, next_block, 0)
    first_step(blocks - 2, [WIDE] * (LANES // WIDE))
    first_step(blocks - 1, [WIDE] * ((2 * LANES - 2 * INNER) // WIDE))
    lax.fori_loop(blocks - 3, blocks - 1, ready_second, 0)
    second_step(blocks - 1, [2 * LANES - 2 * INNER - 2 * STAGE])

    def advance(step):
        def pair(v, carry):
            for odd_step, (now, old) in enumerate(((even, odd), (odd, even))):
                t = 2 * v + odd_step
                step(now, old, step_weights(w_ref, t), t)
            return carry

        lax.fori_loop(0, pairs, pair, 0)

    def inner(now, old, weights, t):
        begin = INNER + STAGE * t
        sweep(now, old, weights, begin, jnp.where(t < 2, 0, cols - 2 * begin))

    advance(inner)
    for f in (0, 1):
        for side in (0, 1):
            col_copy(f, side).wait()


def finish(steps, pairs, even_in, odd_in, w_rows, uo_hbm, vo_hbm, even, odd, u_nat, v_nat, store_sem):
    del even_in, odd_in
    rows, cols = uo_hbm.shape
    blocks = cols // LANES

    def weights_of(t):
        return [w_rows[t, pl.ds(k, 1), :] for k in range(TAPS)]

    def pair(v, carry, extra):
        for odd_step, (now, old) in enumerate(((even, odd), (odd, even))):
            wide_sweep(now, old, weights_of(2 * v + odd_step), cols, extra)
        return carry

    for place in (MARGIN - steps, MARGIN + cols):
        words = pl.ds(place, steps)
        even[0, words, :] = pltpu.roll(even[PLANES, words, :], 1, 1)
        even[PLANES + 1, words, :] = pltpu.roll(even[1, words, :], LANES - 1, 1)

    for t in range(2 * pairs):
        now, old = ((even, odd), (odd, even))[t % 2]
        end = INNER + STAGE * t
        width = STAGE * ((end + steps - 1 - t + STAGE - 1) // STAGE)
        widths = [WIDE] * (width // WIDE - 1)
        widths.append(width - sum(widths))

        def side(i, carry, now=now, old=old, t=t, end=end, width=width, widths=widths):
            left = MARGIN + end - width + i * (cols - 2 * end + width)
            chunk(now, old, weights_of(t), pl.multiple_of(left, 8), widths, False, True)
            return carry

        lax.fori_loop(0, 2, side, 0)

    t = 2 * pairs
    while steps - t > 2:
        extra = 8 * ((steps - 1 - t + 7) // 8)
        until = min(steps - 2, steps - 1 - (extra - 8))
        until += until % 2
        until = min(until, steps - 2)
        lax.fori_loop(t // 2, until // 2, functools.partial(pair, extra=extra), 0)
        t = until
    wide_sweep(even, odd, weights_of(steps - 2), cols, 8)

    last = weights_of(steps - 1)

    def store(f, q):
        src, dst = ((u_nat, uo_hbm), (v_nat, vo_hbm))[f]
        return pltpu.make_async_copy(
            src.at[q, pl.ds(HALO, rows), :],
            dst.at[:, pl.ds(q * LANES, LANES)], store_sem.at[f, q])

    def step(q):
        chunk(odd, even, last, MARGIN + q * LANES, [WIDE] * (LANES // WIDE), False, False)

    def write(q):
        words = pl.ds(MARGIN + q * LANES, LANES)
        for s in range(PLANES):
            lines = pl.ds(s, LANES, stride=PLANES)
            u_now = even[s + 1, words, :]
            u_nat[q, lines, :] = jnp.transpose(4.0 * u_now)
            v_nat[q, lines, :] = jnp.transpose(8.0 * (u_now - odd[s + 1, words, :]))
        for f in (0, 1):
            store(f, q).start()

    step(0)
    for q in range(1, blocks):
        step(q)
        write(q - 1)
    write(blocks - 1)
    for q in range(blocks):
        for f in (0, 1):
            store(f, q).wait()


def solution(mesh):
    n_row, n_col = mesh.shape["row"], mesh.shape["col"]
    tile_spec = P(("ens", "row"), "col")

    def local_run(u_tile, v_tile, stencil_w):
        rows, cols = u_tile.shape
        steps = stencil_w.shape[0]
        blocks = cols // LANES
        assert rows + 2 * HALO == LANES * PLANES and steps % 2 == 0 and steps < HALO
        native = pltpu.VMEM((blocks, rows + 2 * HALO, LANES), jnp.float32)
        level = jax.ShapeDtypeStruct((PLANES + 2, cols + 2 * MARGIN, LANES), jnp.float32)
        hbm, vmem = pl.BlockSpec(memory_space=pltpu.HBM), pl.BlockSpec(memory_space=pltpu.VMEM)
        tile = jax.ShapeDtypeStruct((rows, cols), jnp.float32)
        dma = pltpu.SemaphoreType.DMA
        pairs = min(7, steps // 4, (cols - 2 * INNER - 128) // (4 * STAGE))
        w_rows = jax.ShapeDtypeStruct((steps, 8, LANES), jnp.float32)
        state = pl.pallas_call(
            functools.partial(start, n_row, n_col, steps, pairs),
            out_shape=(level, level, w_rows),
            in_specs=[hbm, hbm, hbm],
            out_specs=(vmem, vmem, vmem),
            scratch_shapes=[
                native, native, pltpu.SMEM((3, 3, steps), jnp.float32), dma((2, blocks)), dma(()),
                dma((2, 2, blocks)), dma((2, 2, blocks)), dma((2, 2)), dma((2, 2)),
            ],
            compiler_params=pltpu.CompilerParams(
                collective_id=0, has_side_effects=True, vmem_limit_bytes=26 * 2**20),
            name="start",
        )(*(pltpu.with_memory_space_constraint(x, pltpu.HBM) for x in (u_tile, v_tile, jnp.transpose(stencil_w, (1, 2, 0)))))
        return pl.pallas_call(
            functools.partial(finish, steps, pairs),
            out_shape=(tile, tile, level, level),
            in_specs=[vmem, vmem, vmem],
            out_specs=(hbm, hbm, vmem, vmem),
            input_output_aliases={0: 2, 1: 3},
            scratch_shapes=[native, native, dma((2, blocks))],
            compiler_params=pltpu.CompilerParams(vmem_limit_bytes=26 * 2**20),
            name="finish",
        )(*state)[:2]

    return jax.shard_map(
        local_run, mesh=mesh, in_specs=(tile_spec, tile_spec, P()), out_specs=(tile_spec, tile_spec), check_vma=False)
```

```python
import functools

import jax
import jax.numpy as jnp
from jax import lax
from jax.experimental import pallas as pl
from jax.experimental.pallas import tpu as pltpu
from jax.sharding import PartitionSpec as P

LANES = 128
PLANES = 9
HALO = 64
MARGIN = 128
INNER = 96
STAGE = 16
WIDE = 32
PARTS = 2
BLOCKS = (8, 4, 1)
TAPS = 5


def step_weights(w_ref, t):
    return (
        1.5 + 0.5 * w_ref[1, 1, t],
        0.5 * w_ref[0, 0, t],
        0.5 * w_ref[0, 1, t],
        0.5 * w_ref[0, 2, t],
        0.5 * w_ref[1, 0, t],
    )


def chunk(now, old, weights, start, widths, left_ghosts, own_ghosts):
    centre, w00, w01, w02, w10 = weights
    blocks = [(sum(widths[:i]), width) for i, width in enumerate(widths)]

    def taps(block, p):
        return [now[p, pl.ds(start + (block[0] + d), block[1]), :] for d in (-1, 0, 1)]

    def update(block, p, up, mid, down):
        cols = pl.ds(start + block[0], block[1])
        new = (
            (centre * mid[1] - old[p, cols, :])
            + w01 * (up[1] + down[1])
            + w10 * (mid[0] + mid[2])
            + w00 * (up[0] + down[2])
            + w02 * (up[2] + down[0])
        )
        old[p, cols, :] = new
        return new

    ghosts = []
    if left_ghosts:
        cols = pl.ds(start - WIDE, WIDE)
        ghosts.append((cols, pltpu.roll(old[PLANES, cols, :], 1, 1), pltpu.roll(old[1, cols, :], LANES - 1, 1)))
    for b in blocks:
        cols = pl.ds(start + b[0], b[1])
        last = update(b, PLANES, taps(b, PLANES - 1), taps(b, PLANES), taps(b, PLANES + 1))
        first = update(b, 1, taps(b, 0), taps(b, 1), taps(b, 2))
        if own_ghosts:
            ghosts.append((cols, pltpu.roll(last, 1, 1), pltpu.roll(first, LANES - 1, 1)))
    for b in blocks:
        up, mid = taps(b, 1), taps(b, 2)
        for p in range(2, PLANES):
            down = taps(b, p + 1)
            update(b, p, up, mid, down)
            up, mid = mid, down
    for cols, top, bottom in ghosts:
        old[0, cols, :] = top
        old[PLANES + 1, cols, :] = bottom


def sweep(now, old, weights, first_col, width):
    done = first_col + MARGIN
    left = width
    counts = []
    for blocks in BLOCKS:
        counts.append((blocks, lax.div(left, WIDE * blocks)))
        left = left - counts[-1][1] * (WIDE * blocks)
    for blocks, count in reversed(counts):
        size = WIDE * blocks

        def body(i, carry, done=done, blocks=blocks, size=size):
            chunk(now, old, weights, pl.multiple_of(done + i * size, 8), [WIDE] * blocks, True, blocks > 1)
            return carry

        lax.fori_loop(0, count, body, 0)
        done = done + count * size


def wide_sweep(now, old, weights, cols, extra):
    part = (cols + 2 * extra) // PARTS
    widths = [WIDE] * (part // WIDE - 1)
    widths.append(part - sum(widths))

    def body(i, carry):
        chunk(now, old, weights, pl.multiple_of(MARGIN - extra + i * part, 8), widths, False, True)
        return carry

    lax.fori_loop(0, PARTS, body, 0)


def start(n_row, n_col, steps, pairs, u_hbm, v_hbm, w_hbm, even, odd, w_rows, u_nat, v_nat, w_ref, load_sem, w_sem,
           row_send, row_recv, col_send, col_recv):
    rows, cols = u_hbm.shape
    blocks = cols // LANES
    row_id, col_id = lax.axis_index("row"), lax.axis_index("col")
    above, below = lax.rem(row_id + n_row - 1, n_row), lax.rem(row_id + 1, n_row)
    left, right = lax.rem(col_id + n_col - 1, n_col), lax.rem(col_id + 1, n_col)

    def load(f, q):
        src, dst = ((u_hbm, u_nat), (v_hbm, v_nat))[f]
        return pltpu.make_async_copy(
            src.at[:, pl.ds(q * LANES, LANES)], dst.at[q, pl.ds(HALO, rows), :], load_sem.at[f, q])

    def row_copy(f, side, q):
        ref = (u_nat, v_nat)[f]
        depth = steps
        lines = (HALO + rows - depth, HALO)[side]
        place = (HALO - depth, HALO + rows)[side]
        return pltpu.make_async_remote_copy(
            src_ref=ref.at[q, pl.ds(lines, depth), :], dst_ref=ref.at[q, pl.ds(place, depth), :],
            send_sem=row_send.at[f, side, q], recv_sem=row_recv.at[f, side, q],
            device_id={"row": (below, above)[side]}, device_id_type=pl.DeviceIdType.MESH)

    def col_copy(f, side):
        ref, planes = (even, odd)[f], pl.ds(1, PLANES)
        depth = steps
        lines = (MARGIN + cols - depth, MARGIN)[side]
        place = (MARGIN - depth, MARGIN + cols)[side]
        return pltpu.make_async_remote_copy(
            src_ref=ref.at[planes, pl.ds(lines, depth), :], dst_ref=ref.at[planes, pl.ds(place, depth), :],
            send_sem=col_send.at[f, side], recv_sem=col_recv.at[f, side],
            device_id={"col": (right, left)[side]}, device_id_type=pl.DeviceIdType.MESH)

    load_weights = pltpu.make_async_copy(w_hbm, w_ref, w_sem)
    load_weights.start()
    order = [0, blocks - 1] + list(range(1, blocks - 1))
    for q in order:
        for f in (0, 1):
            load(f, q).start()

    barrier = pltpu.get_barrier_semaphore()
    for peer in ({"row": above}, {"row": below}, {"col": left}, {"col": right}):
        pl.semaphore_signal(barrier, inc=1, device_id=peer, device_id_type=pl.DeviceIdType.MESH)
    pl.semaphore_wait(barrier, 4)

    for q in order:
        for f in (0, 1):
            load(f, q).wait()
            for side in (0, 1):
                row_copy(f, side, q).start()

    load_weights.wait()

    def spread(t, carry):
        for k, weight in enumerate(step_weights(w_ref, t)):
            w_rows[t, pl.ds(k, 1), :] = jnp.full((1, LANES), weight, jnp.float32)
        return carry

    lax.fori_loop(0, steps, spread, 0)

    def take_rows(q):
        for f in (0, 1):
            for side in (0, 1):
                row_copy(f, side, q).wait()

    def lay_out(q):
        words = pl.ds(pl.multiple_of(MARGIN + q * LANES, LANES), LANES)
        for s in range(PLANES):
            lines = pl.ds(s, LANES, stride=PLANES)
            u_now = 0.25 * u_nat[q, lines, :]
            u_old = u_now - 0.125 * v_nat[q, lines, :]
            u_now = jnp.transpose(u_now)
            even[s + 1, words, :] = u_now
            odd[s + 1, words, :] = jnp.transpose(u_old)
            if s == 0:
                even[PLANES + 1, words, :] = pltpu.roll(u_now, LANES - 1, 1)
            if s == PLANES - 1:
                even[0, words, :] = pltpu.roll(u_now, 1, 1)

    def first_step(q, widths):
        begin = pl.multiple_of(MARGIN + INNER + (q - 1) * LANES, 8)
        chunk(even, odd, step_weights(w_ref, 0), begin, widths, False, True)

    def second_step(q, widths):
        begin = pl.multiple_of(MARGIN + INNER + STAGE + (q - 1) * LANES, 8)
        chunk(odd, even, step_weights(w_ref, 1), begin, widths, False, True)

    take_rows(0)
    lay_out(0)
    take_rows(blocks - 1)
    for f in (0, 1):
        col_copy(f, 1).start()
    lay_out(blocks - 1)
    take_rows(1)
    for f in (0, 1):
        col_copy(f, 0).start()
    lay_out(1)

    def ready_step(q, carry):
        first_step(q, [WIDE] * (LANES // WIDE))
        return carry

    def ready_second(q, carry):
        second_step(q, [WIDE] * (LANES // WIDE))
        return carry

    def next_block(q, carry):
        lax.fori_loop(q - 1, q, ready_step, 0)
        lax.fori_loop(jnp.where(q == 2, 1, q - 2), q - 1, ready_second, 0)
        take_rows(q)
        lay_out(q)
        return carry

    lax.fori_loop(2, blocks - 1, next_block, 0)
    first_step(blocks - 2, [WIDE] * (LANES // WIDE))
    first_step(blocks - 1, [WIDE] * ((2 * LANES - 2 * INNER) // WIDE))
    lax.fori_loop(blocks - 3, blocks - 1, ready_second, 0)
    second_step(blocks - 1, [2 * LANES - 2 * INNER - 2 * STAGE])

    def advance(step):
        def pair(v, carry):
            for odd_step, (now, old) in enumerate(((even, odd), (odd, even))):
                t = 2 * v + odd_step
                step(now, old, step_weights(w_ref, t), t)
            return carry

        lax.fori_loop(0, pairs, pair, 0)

    def inner(now, old, weights, t):
        begin = INNER + STAGE * t
        sweep(now, old, weights, begin, jnp.where(t < 2, 0, cols - 2 * begin))

    advance(inner)
    for f in (0, 1):
        for side in (0, 1):
            col_copy(f, side).wait()


def finish(steps, pairs, even_in, odd_in, w_rows, uo_hbm, vo_hbm, even, odd, u_nat, v_nat, store_sem):
    del even_in, odd_in
    rows, cols = uo_hbm.shape
    blocks = cols // LANES

    def weights_of(t):
        return [w_rows[t, pl.ds(k, 1), :] for k in range(TAPS)]

    def pair(v, carry, extra):
        for odd_step, (now, old) in enumerate(((even, odd), (odd, even))):
            wide_sweep(now, old, weights_of(2 * v + odd_step), cols, extra)
        return carry

    for place in (MARGIN - steps, MARGIN + cols):
        words = pl.ds(place, steps)
        even[0, words, :] = pltpu.roll(even[PLANES, words, :], 1, 1)
        even[PLANES + 1, words, :] = pltpu.roll(even[1, words, :], LANES - 1, 1)

    for t in range(2 * pairs):
        now, old = ((even, odd), (odd, even))[t % 2]
        end = INNER + STAGE * t
        width = STAGE * ((end + steps - 1 - t + STAGE - 1) // STAGE)
        widths = [WIDE] * (width // WIDE - 1)
        widths.append(width - sum(widths))

        def side(i, carry, now=now, old=old, t=t, end=end, width=width, widths=widths):
            left = MARGIN + end - width + i * (cols - 2 * end + width)
            chunk(now, old, weights_of(t), pl.multiple_of(left, 8), widths, False, True)
            return carry

        lax.fori_loop(0, 2, side, 0)

    t = 2 * pairs
    while steps - t > 2:
        extra = 8 * ((steps - 1 - t + 7) // 8)
        until = min(steps - 2, steps - 1 - (extra - 8))
        until += until % 2
        until = min(until, steps - 2)
        lax.fori_loop(t // 2, until // 2, functools.partial(pair, extra=extra), 0)
        t = until
    wide_sweep(even, odd, weights_of(steps - 2), cols, 8)

    last = weights_of(steps - 1)

    def store(f, q):
        src, dst = ((u_nat, uo_hbm), (v_nat, vo_hbm))[f]
        return pltpu.make_async_copy(
            src.at[q, pl.ds(HALO, rows), :],
            dst.at[:, pl.ds(q * LANES, LANES)], store_sem.at[f, q])

    def step(q):
        chunk(odd, even, last, MARGIN + q * LANES, [WIDE] * (LANES // WIDE), False, False)

    def write(q):
        words = pl.ds(MARGIN + q * LANES, LANES)
        for s in range(PLANES):
            lines = pl.ds(s, LANES, stride=PLANES)
            u_now = even[s + 1, words, :]
            u_nat[q, lines, :] = jnp.transpose(4.0 * u_now)
            v_nat[q, lines, :] = jnp.transpose(8.0 * (u_now - odd[s + 1, words, :]))
        for f in (0, 1):
            store(f, q).start()

    step(0)
    for q in range(1, blocks):
        step(q)
        write(q - 1)
    write(blocks - 1)
    for q in range(blocks):
        for f in (0, 1):
            store(f, q).wait()


def solution(mesh):
    n_row, n_col = mesh.shape["row"], mesh.shape["col"]
    tile_spec = P(("ens", "row"), "col")

    def local_run(u_tile, v_tile, stencil_w):
        rows, cols = u_tile.shape
        steps = stencil_w.shape[0]
        blocks = cols // LANES
        assert rows + 2 * HALO == LANES * PLANES and steps % 2 == 0 and steps < HALO
        native = pltpu.VMEM((blocks, rows + 2 * HALO, LANES), jnp.float32)
        level = jax.ShapeDtypeStruct((PLANES + 2, cols + 2 * MARGIN, LANES), jnp.float32)
        hbm, vmem = pl.BlockSpec(memory_space=pltpu.HBM), pl.BlockSpec(memory_space=pltpu.VMEM)
        tile = jax.ShapeDtypeStruct((rows, cols), jnp.float32)
        dma = pltpu.SemaphoreType.DMA
        pairs = min(8, steps // 4, (cols - 2 * INNER - 128) // (4 * STAGE))
        w_rows = jax.ShapeDtypeStruct((steps, 8, LANES), jnp.float32)
        state = pl.pallas_call(
            functools.partial(start, n_row, n_col, steps, pairs),
            out_shape=(level, level, w_rows),
            in_specs=[hbm, hbm, hbm],
            out_specs=(vmem, vmem, vmem),
            scratch_shapes=[
                native, native, pltpu.SMEM((3, 3, steps), jnp.float32), dma((2, blocks)), dma(()),
                dma((2, 2, blocks)), dma((2, 2, blocks)), dma((2, 2)), dma((2, 2)),
            ],
            compiler_params=pltpu.CompilerParams(
                collective_id=0, has_side_effects=True, vmem_limit_bytes=26 * 2**20),
            name="start",
        )(*(pltpu.with_memory_space_constraint(x, pltpu.HBM) for x in (u_tile, v_tile, jnp.transpose(stencil_w, (1, 2, 0)))))
        return pl.pallas_call(
            functools.partial(finish, steps, pairs),
            out_shape=(tile, tile, level, level),
            in_specs=[vmem, vmem, vmem],
            out_specs=(hbm, hbm, vmem, vmem),
            input_output_aliases={0: 2, 1: 3},
            scratch_shapes=[native, native, dma((2, blocks))],
            compiler_params=pltpu.CompilerParams(vmem_limit_bytes=26 * 2**20),
            name="finish",
        )(*state)[:2]

    return jax.shard_map(
        local_run, mesh=mesh, in_specs=(tile_spec, tile_spec, P()), out_specs=(tile_spec, tile_spec), check_vma=False)
```
